32 devices in a mesh: region: 4 (over x, core), domain: 8 (over z, y).
Axes of the slice: x: 2, y: 2, z: 4, core: 2. Of those that a mesh axis runs over, the one named last changes fastest.
Arguments:
- midpoints: float32 [3, 16384], P(None, ('region', 'domain')), may hold values from 0 to 1, as said below
- line_vectors: float32 [3, 16384], P(None, ('region', 'domain')), may hold values from -0.09375 to 0.09375
- burgers: float32 [3, 16384], P(None, ('region', 'domain')), may hold values from -4 to 4
- destination: int32 [16384, 1], P(('region', 'domain')), may hold values from 0 to 7; in each aligned block of 512 rows (0 to 511, 512 to 1023, ...) at most 128 rows name the same one
- node_ids: int32 [2, 16384], P(None, ('region', 'domain')), may hold values from 0 to 2047
- cell_ids: int32 [16384], P(('region', 'domain')), may hold values from 0 to 127, as said below
- cell_centers: float32 [3, 512], replicated, may hold values from 0 to 1, as said below
Outputs:
- slot_traction: float32 [3, 32768], P(None, ('region', 'domain'))
- nodal_force: float32 [3, 8192], P(None, ('region', 'domain'))
The draws below stay inside these ranges and needn't reach their ends.
Inputs may be any that keep to these rules, and one draw needn't show every extreme that they name: `destination`: among the rows of one device, no domain is named by more than 128 rows, a bound that some block reaches. `cell_ids`: region r is the slab of x from r / 4 to (r + 1) / 4 of the unit cube; its 128 cells are the boxes of a 2 x 4 x (16) grid in that slab, numbered with the last grid index fastest. `cell_centers`: each cell's center lies within its box, within a quarter of the box's width of the box's middle along each dimension. `midpoints`: each segment's midpoint lies within its cell's box.
All inputs are finite; a program needn't handle non-finite values.
Results may differ from the reference program's by a relative error of at most 0.0003.
Values sent between devices are 32-bit elements; how exact they have to be, the bound alone decides.
No kernel may reach another device: no remote copies, remote signals or barrier semaphores. Data moves between devices by JAX's collectives and lax.ppermute only.
A program may use at most 64 MiB of HBM per device.

```python
import math
import jax
import jax.numpy as jnp
import numpy as np
from jax import lax

SEG_DEV = 512
CELLS_REG = 128
CAP = 128
SEGMENTS = 16384
CELLS = 512
NODES_REG = 2048
N_REGION = 4
N_DOMAIN = 8


def grid_centers(key):
    index = jnp.arange(CELLS, dtype=jnp.int32)
    region = index // CELLS_REG
    local = index % CELLS_REG
    depth = CELLS_REG // 8
    grid_x = local // (4 * depth)
    grid_y = local // depth % 4
    grid_z = local % depth
    width_x = 1.0 / (2 * N_REGION)
    width_y = 0.25
    width_z = 1.0 / depth
    base = jnp.stack([((region * 2 + grid_x).astype(jnp.float32) + 0.5) * width_x, (grid_y.astype(jnp.float32) + 0.5) * width_y, (grid_z.astype(jnp.float32) + 0.5) * width_z], axis=0)
    widths = jnp.stack([jnp.full((1,), width_x, jnp.float32), jnp.full((1,), width_y, jnp.float32), jnp.full((1,), width_z, jnp.float32)], axis=0)
    jitter = jax.random.uniform(jax.random.fold_in(key, 7), (3, CELLS), jnp.float32, -0.25, 0.25) * widths
    return (base + jitter, widths)


def local_cells(key):
    return jax.random.randint(jax.random.fold_in(key, 5), (SEGMENTS,), 0, CELLS_REG, dtype=jnp.int32)


def draw_cell_centers(key, part):
    return grid_centers(key)[0]


def draw_cell_ids(key, part):
    return local_cells(key)


def draw_midpoints(key, part):
    centers, widths = grid_centers(key)
    cells = local_cells(key)
    region = jnp.arange(SEGMENTS, dtype=jnp.int32) // (SEG_DEV * N_DOMAIN)
    owner = (region * CELLS_REG + cells).astype(jnp.int32)
    offset = jax.random.uniform(jax.random.fold_in(key, 9), (3, SEGMENTS), jnp.float32, -0.24, 0.24) * widths
    return centers[:, owner] + offset


def with_ends(values, own_key, least, largest):
    place = [jax.random.randint(jax.random.fold_in(own_key, axis), (), 0, length) for axis, length in enumerate(values.shape)]
    widest = values.shape.index(max(values.shape))
    neighbour = place[:widest] + [(place[widest] + 1) % values.shape[widest]] + place[widest + 1:]
    return values.at[tuple(place)].set(least).at[tuple(neighbour)].set(largest)


def levels(stream_key, shape, cuts, low, high):
    loudness, own = 1.0, jax.random.fold_in(stream_key, 6)
    for axis_at, blocks in cuts:
        heights = jnp.exp(jax.random.uniform(jax.random.fold_in(own, axis_at), (blocks,), jnp.float32, low / len(cuts), high / len(cuts)))
        loudness = loudness * jnp.repeat(heights, shape[axis_at] // blocks).reshape([-1 if axis == axis_at else 1 for axis in range(len(shape))])
    return loudness


def shared_out(rng, own, number, rows, amount, top, bound, slope):
    ranking = jax.random.permutation(rng, amount)
    crowded, common = load_shares(amount, rows * top, bound, slope, True), load_shares(amount, rows * top, bound, slope, False)
    places = jnp.arange(amount)

    def named(sizes, offset_by):
        used = int((sizes > 0).sum())
        fixed = max(1, used // 4)
        shifted = fixed + (places - fixed + offset_by * (used - fixed)) % max(1, amount - fixed)
        return jnp.zeros((amount,), jnp.int32).at[ranking[jnp.where(places < fixed, places, shifted)]].set(jnp.asarray(sizes, jnp.int32))

    sizes = jnp.where(number % 4 == 0, named(crowded, number // 4), named(common, number - number // 4 - 1))
    mixed = jax.random.permutation(jax.random.fold_in(own, 3), amount)
    donor, sink = mixed[0:amount // 2 * 2:2], mixed[1:amount // 2 * 2:2]
    margin = jnp.minimum(sizes[donor] - 1, bound - sizes[sink]) // 2
    margin = jnp.where((donor == ranking[0]) | (sink == ranking[0]) | (sizes[sink] == 0), 0, jnp.maximum(margin, 0))
    shifted = jax.random.randint(jax.random.fold_in(own, 4), (amount // 2,), 0, 1 << 20) % (margin + 1)
    sizes = sizes.at[donor].add(-shifted).at[sink].add(shifted)
    labels = jnp.searchsorted(jnp.cumsum(sizes), jnp.arange(rows * top), side="right").astype(jnp.int32)
    table = labels.reshape(top, rows).T
    table = table[jax.random.permutation(jax.random.fold_in(own, 1), rows)]
    offset_by = jax.random.randint(jax.random.fold_in(own, 2), (rows, 1), 0, top)
    return jnp.take_along_axis(table, (jnp.arange(top)[None, :] + offset_by) % top, axis=1)


def load_shares(number_of, total, most, skew, full):
    weights = [(1 << 20) // math.isqrt(grade ** skew) + 1 for grade in range(1, number_of + 1)]
    largest = most if full else min(most, max(-(-total // number_of), total * weights[0] // sum(weights)))
    least = 1 if total - largest >= number_of - 1 else 0
    holding, surplus = [largest] + [least] * (number_of - 1), total - largest - least * (number_of - 1)
    while surplus > 0:
        candidates = [i for i in range(1, number_of) if holding[i] < largest] or [i for i in range(1, number_of) if holding[i] < most]
        pool, left = sum([weights[i] for i in candidates]), surplus
        for i in candidates:
            more = min(most - holding[i], max(1, left * weights[i] // pool), surplus)
            holding[i] = holding[i] + more
            surplus = surplus - more
    return np.array(holding)


def scatter_about(key, shape, scale, most, cuts=(), kind=jnp.bfloat16):
    gain = levels(key, shape, cuts, -0.22, 0.18) if cuts else 1.0
    values = jax.random.normal(key, shape, jnp.float32) * scale * gain
    return jnp.minimum(jnp.maximum(values, -most), most).astype(kind)


def setup_inputs(seed: int = 0) -> dict:
    streams_of = jax.random.split(jax.random.key(seed), 8)
    midpoints = draw_midpoints(jax.random.fold_in(streams_of[7], 71), 0)
    line_vectors = scatter_about(streams_of[1], (3, SEGMENTS), (SEG_DEV * N_DOMAIN) ** -0.5, 0.09375, ((1, 32),), jnp.float32)
    burgers = scatter_about(streams_of[2], (3, SEGMENTS), 1.0, 4.0, ((1, 32),), jnp.float32)
    destination_keys = jax.random.split(jax.random.fold_in(streams_of[3], 1), SEGMENTS // SEG_DEV)
    destination_turns = jax.random.permutation(jax.random.fold_in(streams_of[3], 3), SEGMENTS // SEG_DEV)
    destination = jax.vmap(lambda own, number: shared_out(jax.random.fold_in(streams_of[3], 2), own, number, SEG_DEV, N_DOMAIN, 1, CAP, 2))(destination_keys, destination_turns).reshape((SEGMENTS, 1))
    node_ids = with_ends(jax.random.randint(streams_of[4], (2, SEGMENTS), 0, NODES_REG), jax.random.fold_in(streams_of[4], 1), 0, NODES_REG - 1).astype(jnp.int32)
    cell_ids = draw_cell_ids(jax.random.fold_in(streams_of[7], 71), 0)
    cell_centers = draw_cell_centers(jax.random.fold_in(streams_of[7], 71), 0)
    return dict(midpoints=midpoints, line_vectors=line_vectors, burgers=burgers, destination=destination, node_ids=node_ids, cell_ids=cell_ids, cell_centers=cell_centers)


CORE2 = 0.01
EXACT = lax.Precision.HIGHEST

def product(left, right):
    return jnp.dot(left, right, precision=EXACT, preferred_element_type=jnp.float32)

def source_terms(m, l, b):
    count = m.shape[1]
    outer = (b[:, None, :] * l[None, :, :]).reshape(9, count)
    q = jnp.cross(b, l, axis=0)
    qm = (q[:, None, :] * m[None, :, :]).reshape(9, count)
    return (outer, jnp.concatenate([qm, q], axis=0))

def pair_block(m, outer, second, targets):
    r2 = (targets[0][None, :] - m[0][:, None]) ** 2
    r2 = r2 + (targets[1][None, :] - m[1][:, None]) ** 2
    r2 = r2 + (targets[2][None, :] - m[2][:, None]) ** 2
    g1 = 1.0 / jnp.sqrt(r2 + CORE2)
    g3 = g1 * g1 * g1
    first = product(outer, g1)
    other = product(second, g3)
    cross_part = (other[9:12][:, None, :] * targets[None, :, :]).reshape(9, targets.shape[1])
    return first + cross_part - other[0:9]

def moment_terms(m, l, b, centers):
    count = m.shape[1]
    outer = (b[:, None, :] * l[None, :, :]).reshape(9, count)
    offset = m - centers
    dipole = (outer[:, None, :] * offset[None, :, :]).reshape(27, count)
    q = jnp.cross(b, l, axis=0)
    return jnp.concatenate([outer, dipole, q], axis=0)

def far_field(moments, centers, region_centers, region, cells_reg):
    total = centers.shape[1]
    diffs = [region_centers[a][None, :] - centers[a][:, None] for a in range(3)]
    r2 = diffs[0] ** 2 + diffs[1] ** 2 + diffs[2] ** 2
    keep = (jnp.arange(total, dtype=jnp.int32) // cells_reg != region).astype(jnp.float32)
    g1 = keep[:, None] / jnp.sqrt(r2 + CORE2)
    g3 = g1 * g1 * g1
    field = product(moments[0:9], g1)
    pulls = []
    for axis_a in range(3):
        weighted = diffs[axis_a] * g3
        field = field + product(moments[9 + axis_a:36:3], weighted)
        pulls.append(product(moments[36:39], weighted))
    nterm = jnp.stack(pulls, axis=1).reshape(9, region_centers.shape[1])
    return field + nterm

def traction(stress, b):
    count = stress.shape[1]
    sigma = stress.reshape(3, 3, count)
    sym = 0.5 * (sigma + jnp.transpose(sigma, (1, 0, 2)))
    return lax.optimization_barrier(jnp.sum(sym * b[None, :, :], axis=1))

def reference(midpoints, line_vectors, burgers, destination, node_ids, cell_ids, cell_centers):
    per_region = SEG_DEV * N_DOMAIN
    total = midpoints.shape[1]
    devices = N_REGION * N_DOMAIN
    capacity = 2 * SEG_DEV // N_DOMAIN
    region_of = jnp.arange(total, dtype=jnp.int32) // per_region
    global_cell = (region_of * CELLS_REG + cell_ids).astype(jnp.int32)
    seg_centers = cell_centers[:, global_cell]
    feats = moment_terms(midpoints, line_vectors, burgers, seg_centers)
    moments = jax.ops.segment_sum(feats.T, global_cell, num_segments=CELLS_REG * N_REGION).T

    def region_traction(region):
        low = (region * per_region).astype(jnp.int32)
        m = lax.dynamic_slice_in_dim(midpoints, low, per_region, 1)
        l = lax.dynamic_slice_in_dim(line_vectors, low, per_region, 1)
        b = lax.dynamic_slice_in_dim(burgers, low, per_region, 1)
        cells = lax.dynamic_slice_in_dim(cell_ids, low, per_region, 0)
        region_centers = lax.dynamic_slice_in_dim(cell_centers, (region * CELLS_REG).astype(jnp.int32), CELLS_REG, 1)
        far = far_field(moments, cell_centers, region_centers, region, CELLS_REG)

        def add_block(total_stress, index):
            start = (index * SEG_DEV).astype(jnp.int32)
            bm = lax.dynamic_slice_in_dim(m, start, SEG_DEV, 1)
            bl = lax.dynamic_slice_in_dim(l, start, SEG_DEV, 1)
            bb = lax.dynamic_slice_in_dim(b, start, SEG_DEV, 1)
            outer, second = source_terms(bm, bl, bb)
            return (total_stress + pair_block(bm, outer, second, m), None)
        near, _ = lax.scan(add_block, jnp.zeros((9, per_region), jnp.float32), jnp.arange(N_DOMAIN, dtype=jnp.int32))
        stress = near + far[:, cells]
        return traction(stress, b)
    tractions = lax.map(region_traction, jnp.arange(N_REGION, dtype=jnp.int32))
    tractions = jnp.transpose(tractions, (1, 0, 2)).reshape(3, total)
    dest = destination[:, 0].reshape(devices, SEG_DEV)
    hot = (dest[:, :, None] == jnp.arange(N_DOMAIN, dtype=jnp.int32)[None, None, :]).astype(jnp.int32)
    rank = lax.optimization_barrier(jnp.sum(jnp.cumsum(hot, axis=1) * hot, axis=2)) - 1
    device = jnp.arange(devices, dtype=jnp.int32)[:, None]
    slot = (device // N_DOMAIN * N_DOMAIN + dest) * (2 * SEG_DEV) + device % N_DOMAIN * capacity + rank
    slot = slot.reshape(total).astype(jnp.int32)
    slot_traction = jnp.zeros((3, 2 * total), jnp.float32).at[:, slot].set(tractions)
    node_global = (region_of[None, :] * NODES_REG + node_ids).astype(jnp.int32)
    half = 0.5 * tractions
    nodal_force = jnp.zeros((3, NODES_REG * N_REGION), jnp.float32)
    nodal_force = nodal_force.at[:, node_global[0]].add(half).at[:, node_global[1]].add(half)
    return (slot_traction, nodal_force)
```

```python
import functools

import jax
import jax.numpy as jnp
from jax import lax
from jax.experimental import pallas as pl
from jax.experimental.pallas import tpu as pltpu
from jax.sharding import PartitionSpec as P

CORE2 = 0.01
LANES = 128
F32 = jnp.float32
BF16 = jnp.bfloat16
SYM = ((0, 0), (1, 1), (2, 2), (0, 1), (0, 2), (1, 2))
SENT = 10
DIST_ROWS, FIRST_ROWS, SECOND_ROWS = 32, 16, 32
NEAR_ROWS = DIST_ROWS + FIRST_ROWS + SECOND_ROWS
MOMENT_ROWS = 32
VMEM_LIMIT = 32 << 20
VMEM_SPEC = pl.BlockSpec(memory_space=pltpu.VMEM)


def rounded(x):
    return x.astype(BF16).astype(F32)


def split2(x):
    high = rounded(x)
    return high, x - high


def split3(x):
    high = rounded(x)
    rest = x - high
    middle = rounded(rest)
    return high, middle, rest - middle


def dot(left, right):
    return jnp.dot(left, right, preferred_element_type=F32)


def dot_nt(left, right):
    return lax.dot_general(left, right, (((1,), (1,)), ((), ())), preferred_element_type=F32)


def middle_of(regions):
    region = lax.axis_index("region")
    return ((region.astype(F32) + 0.5) / regions, 0.5, 0.5)


def call(body, out_shape, inputs, flops, name):
    return pl.pallas_call(
        body,
        out_shape=out_shape,
        in_specs=[VMEM_SPEC] * len(inputs),
        out_specs=jax.tree.map(lambda _: VMEM_SPEC, out_shape),
        cost_estimate=pl.CostEstimate(flops=flops, bytes_accessed=1 << 16, transcendentals=0),
        compiler_params=pltpu.CompilerParams(vmem_limit_bytes=VMEM_LIMIT),
        name=name,
    )(*inputs)


def pack_body(m_ref, l_ref, b_ref, cell_ref, out_ref):
    quarters = m_ref.shape[1] // LANES
    parts = [ref[...] for ref in (m_ref, l_ref, b_ref)] + [cell_ref[...].astype(F32)]
    rows = [
        part[a : a + 1, q * LANES : (q + 1) * LANES]
        for part in parts
        for a in range(part.shape[0])
        for q in range(quarters)
    ]
    block = jnp.concatenate(rows, axis=0)
    for d in range(out_ref.shape[0]):
        out_ref[d] = block


def local_body(regions, domains, m_ref, dest_ref, nodes_ref, cell_ref, centers_ref, target_ref, hot_ref, cell_hot_ref, far_ref):
    count = m_ref.shape[1]
    cells = centers_ref.shape[1] // regions
    region = lax.axis_index("region")
    middle = middle_of(regions)
    x = [m_ref[a : a + 1, :] - middle[a] for a in range(3)]
    parts = [split3(-2.0 * v) for v in x]
    norm = split3(x[0] * x[0] + x[1] * x[1] + x[2] * x[2] + CORE2)
    ones = jnp.ones((1, count), F32)
    rows = [parts[a][p] for a in range(3) for p in (0, 1, 2, 0, 1, 0)]
    rows += [ones, ones, ones] + list(norm) + [jnp.zeros((DIST_ROWS - 24, count), F32)]
    target_ref[...] = jnp.concatenate(rows, axis=0).astype(BF16)
    dest = dest_ref[...]
    hot = (lax.broadcasted_iota(jnp.int32, (domains, count), 0) == dest).astype(BF16)
    earlier = (
        lax.broadcasted_iota(jnp.int32, (count, count), 0)
        < lax.broadcasted_iota(jnp.int32, (count, count), 1)
    ).astype(BF16)
    before = dot(hot, earlier)
    rank = jnp.sum(before * hot.astype(F32), axis=0, keepdims=True).astype(jnp.int32)
    slot = dest * LANES + rank
    ids = jnp.concatenate([slot, nodes_ref[...], jnp.zeros((5, count), jnp.int32)], axis=0).astype(F32)
    columns = jnp.transpose(ids).astype(jnp.int32)
    slots = domains * LANES
    wide = 1024
    for start in range(0, hot_ref.shape[1], wide):
        lane = lax.broadcasted_iota(jnp.int32, (count, wide), 1) + (start % slots if start < slots else start - slots)
        if start < slots:
            value = (lane == columns[:, 0:1]).astype(F32)
        else:
            value = 0.5 * (lane == columns[:, 1:2]).astype(F32) + 0.5 * (lane == columns[:, 2:3]).astype(F32)
        hot_ref[:, start : start + wide] = value.astype(BF16)
    cell_hot_ref[...] = (lax.broadcasted_iota(jnp.int32, (cells, count), 0) == cell_ref[...]).astype(BF16)
    here = centers_ref[:, pl.ds(pl.multiple_of(region * cells, cells), cells)]
    for k in range(1, regions):
        other = lax.bitwise_xor(region, k)
        there = centers_ref[:, pl.ds(pl.multiple_of(other * cells, cells), cells)]
        column = jnp.transpose(jnp.concatenate([there, jnp.zeros((5, cells), F32)], axis=0))
        d = [here[a : a + 1, :] - column[:, a : a + 1] for a in range(3)]
        g1 = lax.rsqrt(d[0] * d[0] + d[1] * d[1] + d[2] * d[2] + CORE2)
        g3 = g1 * g1 * g1
        for j, factor in enumerate([g1] + [v * g3 for v in d]):
            high, low = split2(factor)
            row = ((k - 1) * 4 + j) * cells
            far_ref[row : row + cells, 0:cells] = high.astype(BF16)
            far_ref[row : row + cells, cells : 2 * cells] = low.astype(BF16)


def source_body(regions, got_ref, centers_ref, near_ref, moment_ref, terms_ref, cell_rows_ref):
    sent_rows = SENT * 4
    devices = got_ref.shape[0] // sent_rows
    cells = moment_ref.shape[1]
    middle = middle_of(regions)
    zero = jnp.zeros((8, LANES), F32)
    one = jnp.ones((8, LANES), F32)
    quarters = 4
    for group in range(devices // 8):
        for quarter in range(quarters):

            def value(c):
                return got_ref[pl.ds(group * 8 * sent_rows + c * quarters + quarter, 8, stride=sent_rows), :]

            first_block = (group * quarters + quarter) * 8
            m = [value(a) - middle[a] for a in range(3)]
            l = [value(3 + a) for a in range(3)]
            b = [value(6 + a) for a in range(3)]
            q = [b[1] * l[2] - b[2] * l[1], b[2] * l[0] - b[0] * l[2], b[0] * l[1] - b[1] * l[0]]
            outer = [b[i] * l[i] if i == j else 0.5 * (b[i] * l[j] + b[j] * l[i]) for i, j in SYM]
            second = q + [q[i] * m[i] if i == j else 0.5 * (q[i] * m[j] + q[j] * m[i]) for i, j in SYM]
            parts = [split3(v) for v in m]
            norm = split3(m[0] * m[0] + m[1] * m[1] + m[2] * m[2])
            rows = [parts[a][p] for a in range(3) for p in (0, 0, 0, 1, 1, 2)]
            rows += list(norm) + [one, one, one] + [zero] * (DIST_ROWS - 24)
            pair = [split2(v) for v in outer]
            for p in range(2):
                rows += [v[p] for v in pair] + [None] * (FIRST_ROWS // 2 - 6)
            pair = [split2(v) for v in second]
            for p in range(2):
                rows += [v[p] for v in pair] + [None] * (SECOND_ROWS // 2 - 9)
            for f, row in enumerate(rows):
                near_ref[pl.ds(first_block * NEAR_ROWS + f, 8, stride=NEAR_ROWS), :] = zero if row is None else row
            terms = outer + [q[0], q[1]]
            for a in range(3):
                terms += [v * m[a] for v in outer] + ([q[2], zero] if a == 0 else [zero, zero])
            terms = [split3(v) for v in terms]
            for p in range(3):
                for f, row in enumerate(terms):
                    at = first_block * 3 * MOMENT_ROWS + p * MOMENT_ROWS + f
                    terms_ref[pl.ds(at, 8, stride=3 * MOMENT_ROWS), :] = row[p]
            cell_rows_ref[first_block : first_block + 8, :] = value(9).astype(jnp.int32)

    def step(i, total):
        left = [terms_ref[pl.ds(pl.multiple_of((2 * i + h) * 3 * MOMENT_ROWS, 8), 3 * MOMENT_ROWS), :] for h in range(2)]
        left = jnp.concatenate(left, axis=1).astype(BF16)
        rows = [cell_rows_ref[pl.ds(2 * i + h, 1), :] for h in range(2)]
        hot = jnp.concatenate(rows, axis=1) == lax.broadcasted_iota(jnp.int32, (cells, 2 * LANES), 0)
        return total + dot_nt(left, hot.astype(BF16))

    blocks = devices * quarters
    total = lax.fori_loop(0, blocks // 2, step, jnp.zeros((3 * MOMENT_ROWS, cells), F32), unroll=4)
    total = total[0:32] + total[32:64] + total[64:96]
    region = lax.axis_index("region")
    here = centers_ref[:, pl.ds(pl.multiple_of(region * cells, cells), cells)]
    charge = total[0:6]
    n = [total[6:7], total[7:8], total[14:15]]
    none = jnp.zeros((1, cells), F32)
    fold = [
        [n[0], none, none, 0.5 * n[1], 0.5 * n[2], none],
        [none, n[1], none, 0.5 * n[0], none, 0.5 * n[2]],
        [none, none, n[2], none, 0.5 * n[0], 0.5 * n[1]],
    ]
    pad = jnp.zeros((2, cells), F32)
    moment_ref[0:8, :] = jnp.concatenate([charge, pad], axis=0)
    for a in range(3):
        about = total[8 + 8 * a : 14 + 8 * a] - (here[a : a + 1, :] - middle[a]) * charge
        about = about + jnp.concatenate(fold[a], axis=0)
        moment_ref[8 + 8 * a : 16 + 8 * a, :] = jnp.concatenate([about, pad], axis=0)


def near_body(near_ref, target_ref, first_ref, second_ref):
    blocks = near_ref.shape[0] // NEAR_ROWS
    count = target_ref.shape[1]
    first_ref[...] = jnp.zeros_like(first_ref)
    second_ref[...] = jnp.zeros_like(second_ref)

    def step(i, carry):
        part = [near_ref[pl.ds(pl.multiple_of((2 * i + h) * NEAR_ROWS, 8), NEAR_ROWS), :] for h in range(2)]
        factors = jnp.concatenate([jnp.transpose(p[0:DIST_ROWS]) for p in part], axis=0).astype(BF16)
        rows = jnp.concatenate([p[DIST_ROWS:] for p in part], axis=1).astype(BF16)
        for start in range(0, count, 256):
            at = slice(start, start + 256)
            g1 = lax.rsqrt(dot(factors, target_ref[:, at]))
            g3 = g1 * g1 * g1
            high = g1.astype(BF16)
            low = (g1 - high.astype(F32)).astype(BF16)
            first_ref[:, at] += dot(rows[0:FIRST_ROWS], high) + dot(rows[0:FIRST_ROWS], low)
            high = g3.astype(BF16)
            low = (g3 - high.astype(F32)).astype(BF16)
            second_ref[:, at] += dot(rows[FIRST_ROWS:], high) + dot(rows[FIRST_ROWS:], low)
        return carry

    lax.fori_loop(0, blocks // 2, step, 0, unroll=2)


def stacked3(x):
    return jnp.concatenate(split3(x), axis=0).astype(BF16)


def force_body(regions, m_ref, b_ref, first_ref, second_ref, far_ref, cell_hot_ref, hot_ref, *rest):
    moment_refs, out_ref = rest[:-1], rest[-1]
    cells = moment_refs[0].shape[1]
    domains = out_ref.shape[0]
    middle = middle_of(regions)
    left = [ref[8 * j : 8 * j + 8, :] for ref in moment_refs for j in range(4)]
    left = stacked3(jnp.concatenate(left, axis=1))
    field = dot(left, far_ref[...])
    field = field[:, 0:cells] + field[:, cells:]
    field = field[0:8] + field[8:16] + field[16:24]
    field = dot(stacked3(field), cell_hot_ref[...])
    field = field[0:8] + field[8:16] + field[16:24]
    first = first_ref[...]
    second = second_ref[...]
    second = second[0:16] + second[16:32]
    x = [m_ref[a : a + 1, :] - middle[a] for a in range(3)]
    q = [second[a : a + 1] for a in range(3)]
    cross = [q[i] * x[i] if i == j else 0.5 * (q[i] * x[j] + q[j] * x[i]) for i, j in SYM]
    sigma = first[0:6] + first[8:14] + (jnp.concatenate(cross, axis=0) - second[3:9]) + field[0:6]
    at = {}
    for row, (i, j) in enumerate(SYM):
        at[i, j] = at[j, i] = sigma[row : row + 1]
    b = [b_ref[a : a + 1, :] for a in range(3)]
    force = [at[i, 0] * b[0] + at[i, 1] * b[1] + at[i, 2] * b[2] for i in range(3)]
    force = jnp.concatenate(force + [jnp.zeros((5, b[0].shape[1]), F32)], axis=0)
    spread = dot(stacked3(force), hot_ref[...])
    spread = spread[0:3] + spread[8:11] + spread[16:19]
    slots = domains * LANES
    own = (spread.shape[1] - slots) // domains
    for d in range(domains):
        pieces = [spread[:, d * LANES : (d + 1) * LANES]]
        for h in range(own // LANES):
            pieces.append(spread[:, slots + d * own + h * LANES : slots + d * own + (h + 1) * LANES])
        used = 3 * len(pieces)
        pieces.append(jnp.zeros((out_ref.shape[1] - used, LANES), F32))
        out_ref[d] = jnp.concatenate(pieces, axis=0)


def collect_body(got_ref, slot_ref, node_ref):
    domains = got_ref.shape[0]
    capacity = slot_ref.shape[1] // domains
    total = jnp.sum(got_ref[...], axis=0)
    for d in range(domains):
        slot_ref[:, d * capacity : (d + 1) * capacity] = got_ref[d, 0:3, 0:capacity]
    for h in range(node_ref.shape[1] // LANES):
        node_ref[:, h * LANES : (h + 1) * LANES] = total[3 + 3 * h : 6 + 3 * h]


def body(midpoints, line_vectors, burgers, destination, node_ids, cell_ids, cell_centers):
    count = midpoints.shape[1]
    domains = lax.axis_size("domain")
    regions = lax.axis_size("region")
    cells = cell_centers.shape[1] // regions
    nodes = count // 2 * domains
    own = nodes // domains
    cell_row = cell_ids.reshape(1, count)
    dest_row = destination.reshape(1, count)
    shape = jax.ShapeDtypeStruct
    quarters = count // LANES
    payload = call(
        pack_body,
        shape((domains, SENT * quarters, LANES), F32),
        (midpoints, line_vectors, burgers, cell_row),
        1 << 12,
        "pack",
    )
    got = lax.all_to_all(payload, "domain", split_axis=0, concat_axis=0, tiled=True)
    far_rows = (regions - 1) * 4 * cells
    target, hot, cell_hot, far = call(
        functools.partial(local_body, regions, domains),
        (
            pltpu.VMEM((DIST_ROWS, count), BF16),
            pltpu.VMEM((count, domains * LANES + nodes), BF16),
            pltpu.VMEM((cells, count), BF16),
            pltpu.VMEM((far_rows, 2 * cells), BF16),
        ),
        (midpoints, dest_row, node_ids, cell_row, cell_centers),
        1 << 30,
        "local",
    )
    blocks = domains * quarters
    near, moments = pl.pallas_call(
        functools.partial(source_body, regions),
        out_shape=(pltpu.VMEM((blocks * NEAR_ROWS, LANES), F32), shape((MOMENT_ROWS, cells), F32)),
        in_specs=[VMEM_SPEC] * 2,
        out_specs=(VMEM_SPEC, VMEM_SPEC),
        scratch_shapes=[
            pltpu.VMEM((blocks * 3 * MOMENT_ROWS, LANES), F32),
            pltpu.VMEM((blocks, LANES), jnp.int32),
        ],
        cost_estimate=pl.CostEstimate(flops=1 << 28, bytes_accessed=1 << 16, transcendentals=0),
        compiler_params=pltpu.CompilerParams(vmem_limit_bytes=VMEM_LIMIT),
        name="sources",
    )(got.reshape(domains * SENT * quarters, LANES), cell_centers)
    others = [
        lax.ppermute(moments, "region", [(r, r ^ k) for r in range(regions)]) for k in range(1, regions)
    ]
    first, second = call(
        near_body,
        (pltpu.VMEM((FIRST_ROWS, count), F32), pltpu.VMEM((SECOND_ROWS, count), F32)),
        (near, target),
        1 << 32,
        "near",
    )
    rows = -(-(3 + 3 * (own // LANES)) // 8) * 8
    outgoing = call(
        functools.partial(force_body, regions),
        shape((domains, rows, LANES), F32),
        (midpoints, burgers, first, second, far, cell_hot, hot, *others),
        1 << 28,
        "force",
    )
    arrived = lax.all_to_all(outgoing, "domain", split_axis=0, concat_axis=0, tiled=True)
    return call(
        collect_body,
        (shape((3, 2 * count), F32), shape((3, own), F32)),
        (arrived,),
        1 << 12,
        "collect",
    )


def solution(mesh):
    both = ("region", "domain")
    in_specs = (P(None, both), P(None, both), P(None, both), P(both, None), P(None, both), P(both), P())
    out_specs = (P(None, both), P(None, both))
    return jax.shard_map(body, mesh=mesh, in_specs=in_specs, out_specs=out_specs, check_vma=False)
```

```python
import functools

import jax
import jax.numpy as jnp
from jax import lax
from jax.experimental import pallas as pl
from jax.experimental.pallas import tpu as pltpu
from jax.sharding import PartitionSpec as P

CORE2 = 0.01
LANES = 128
F32 = jnp.float32
BF16 = jnp.bfloat16
SYM = ((0, 0), (1, 1), (2, 2), (0, 1), (0, 2), (1, 2))
SENT = 10
SOURCE_ROWS = 24
DIST_ROWS = 48
FIRST_ROWS, SECOND_ROWS = 16, 32
PIPELINE = 16
MOMENT_ROWS = 32
VMEM_LIMIT = 16 << 20
VMEM_SPEC = pl.BlockSpec(memory_space=pltpu.VMEM)


def rounded(x):
    return x.astype(BF16).astype(F32)


def split2(x):
    high = rounded(x)
    return high, x - high


def split3(x):
    high = rounded(x)
    rest = x - high
    middle = rounded(rest)
    return high, middle, rest - middle


def dot(left, right):
    return jnp.dot(left, right, preferred_element_type=F32)


def dot_nt(left, right):
    return lax.dot_general(left, right, (((1,), (1,)), ((), ())), preferred_element_type=F32)


def middle_of(regions):
    region = lax.axis_index("region")
    return ((region.astype(F32) + 0.5) / regions, 0.5, 0.5)


def call(body, out_shape, inputs, flops, name, scratch=(), fetched=()):
    space = pl.BlockSpec(memory_space=pltpu.HBM) if fetched else VMEM_SPEC
    if fetched:
        inputs = [pltpu.with_memory_space_constraint(x, pltpu.HBM) for x in inputs]
    scratch = list(scratch) + [pltpu.VMEM(x.shape, x.dtype) for x in fetched]
    if fetched:
        scratch.append(pltpu.SemaphoreType.DMA((len(fetched),)))
    return pl.pallas_call(
        body,
        out_shape=out_shape,
        in_specs=[space] * len(inputs),
        out_specs=jax.tree.map(lambda _: VMEM_SPEC, out_shape),
        scratch_shapes=scratch,
        cost_estimate=pl.CostEstimate(flops=flops, bytes_accessed=1 << 16, transcendentals=0),
        compiler_params=pltpu.CompilerParams(vmem_limit_bytes=VMEM_LIMIT),
        name=name,
    )(*inputs)


def fetch(sources, buffers, semaphores):
    copies = [pltpu.make_async_copy(s, t, semaphores.at[i]) for i, (s, t) in enumerate(zip(sources, buffers))]
    for copy in copies:
        copy.start()
    for copy in copies:
        copy.wait()


def pack_body(*refs):
    sources, out_ref, buffers, semaphores = refs[:4], refs[4], refs[5:9], refs[9]
    fetch(sources, buffers, semaphores)
    m_ref, l_ref, b_ref, cell_ref = buffers
    quarters = m_ref.shape[1] // LANES
    parts = [ref[...] for ref in (m_ref, l_ref, b_ref)] + [cell_ref[...].astype(F32)]
    rows = [
        part[a : a + 1, q * LANES : (q + 1) * LANES]
        for part in parts
        for a in range(part.shape[0])
        for q in range(quarters)
    ]
    block = jnp.concatenate(rows, axis=0)
    for d in range(out_ref.shape[0]):
        out_ref[d] = block


def local_body(regions, domains, *refs):
    sources, outputs, buffers, semaphores = refs[:5], refs[5:9], refs[9:14], refs[14]
    fetch(sources, buffers, semaphores)
    m_ref, dest_ref, nodes_ref, cell_ref, centers_ref = buffers
    target_ref, hot_ref, cell_hot_ref, far_ref = outputs
    count = m_ref.shape[1]
    cells = centers_ref.shape[1] // regions
    region = lax.axis_index("region")
    middle = middle_of(regions)
    x = [m_ref[a : a + 1, :] - middle[a] for a in range(3)]
    parts = [split3(-2.0 * v) for v in x]
    norm = split3(x[0] * x[0] + x[1] * x[1] + x[2] * x[2] + CORE2)
    one, none, pad = jnp.ones((1, count), F32), jnp.zeros((1, count), F32), jnp.zeros((3, count), F32)
    rows = []
    for p, of_source, of_target in ((0, one, norm[0]), (1, none, norm[1]), (2, none, norm[2]), (0, one, none), (1, none, none), (0, one, none)):
        rows += [parts[0][p], parts[1][p], parts[2][p], of_source, of_target, pad]
    target_ref[...] = jnp.concatenate(rows, axis=0).astype(BF16)
    dest = dest_ref[...]
    hot = (lax.broadcasted_iota(jnp.int32, (domains, count), 0) == dest).astype(BF16)
    earlier = (
        lax.broadcasted_iota(jnp.int32, (count, count), 0)
        < lax.broadcasted_iota(jnp.int32, (count, count), 1)
    ).astype(BF16)
    before = dot(hot, earlier)
    rank = jnp.sum(before * hot.astype(F32), axis=0, keepdims=True).astype(jnp.int32)
    slot = dest * LANES + rank
    ids = jnp.concatenate([slot, nodes_ref[...], jnp.zeros((5, count), jnp.int32)], axis=0).astype(F32)
    columns = jnp.transpose(ids).astype(jnp.int32)
    slots = domains * LANES
    wide = 1024
    for start in range(0, hot_ref.shape[1], wide):
        lane = lax.broadcasted_iota(jnp.int32, (count, wide), 1) + (start % slots if start < slots else start - slots)
        if start < slots:
            value = (lane == columns[:, 0:1]).astype(F32)
        else:
            value = 0.5 * (lane == columns[:, 1:2]).astype(F32) + 0.5 * (lane == columns[:, 2:3]).astype(F32)
        hot_ref[:, start : start + wide] = value.astype(BF16)
    cell_hot_ref[...] = (lax.broadcasted_iota(jnp.int32, (cells, count), 0) == cell_ref[...]).astype(BF16)
    here = centers_ref[:, pl.ds(pl.multiple_of(region * cells, cells), cells)]
    for k in range(1, regions):
        other = lax.bitwise_xor(region, k)
        there = centers_ref[:, pl.ds(pl.multiple_of(other * cells, cells), cells)]
        column = jnp.transpose(jnp.concatenate([there, jnp.zeros((5, cells), F32)], axis=0))
        d = [here[a : a + 1, :] - column[:, a : a + 1] for a in range(3)]
        g1 = lax.rsqrt(d[0] * d[0] + d[1] * d[1] + d[2] * d[2] + CORE2)
        g3 = g1 * g1 * g1
        for j, factor in enumerate([g1] + [v * g3 for v in d]):
            high, low = split2(factor)
            row = ((k - 1) * 4 + j) * cells
            far_ref[row : row + cells, 0:cells] = high.astype(BF16)
            far_ref[row : row + cells, cells : 2 * cells] = low.astype(BF16)


def source_body(regions, got_ref, centers_ref, near_ref, moment_ref):
    quarters = 4
    sent_rows = SENT * quarters
    devices = got_ref.shape[0] // sent_rows
    cells = moment_ref.shape[1]
    middle = middle_of(regions)
    zero = jnp.zeros((8, LANES), F32)
    one = jnp.ones((8, LANES), F32)
    for group in range(devices // 8):
        for quarter in range(quarters):

            def value(c):
                return got_ref[pl.ds(group * 8 * sent_rows + c * quarters + quarter, 8, stride=sent_rows), :]

            first_block = (group * quarters + quarter) * 8
            m = [value(a) - middle[a] for a in range(3)]
            l = [value(3 + a) for a in range(3)]
            b = [value(6 + a) for a in range(3)]
            q = [b[1] * l[2] - b[2] * l[1], b[2] * l[0] - b[0] * l[2], b[0] * l[1] - b[1] * l[0]]
            outer = [b[i] * l[i] if i == j else 0.5 * (b[i] * l[j] + b[j] * l[i]) for i, j in SYM]
            second = [q[i] * m[i] if i == j else 0.5 * (q[i] * m[j] + q[j] * m[i]) for i, j in SYM]
            norm = m[0] * m[0] + m[1] * m[1] + m[2] * m[2]
            rows = m + [norm, one, value(9), zero, zero] + outer + q + second + [zero]
            for f, row in enumerate(rows):
                near_ref[pl.ds(first_block * SOURCE_ROWS + f, 8, stride=SOURCE_ROWS), :] = row

    def step(i, total):
        left, rows = [], []
        for h in range(2):
            part = near_ref[pl.ds(pl.multiple_of((2 * i + h) * SOURCE_ROWS, 8), SOURCE_ROWS), :]
            plain = part[8:16]
            terms = [split3(v) for v in [plain] + [plain * part[a : a + 1] for a in range(3)] + [part[16:24]]]
            left.append(jnp.concatenate([t[p] for p in range(3) for t in terms], axis=0))
            rows.append(part[5:6])
        left = jnp.concatenate(left, axis=1).astype(BF16)
        row = jnp.concatenate(rows, axis=1).astype(jnp.int32)
        hot = row == lax.broadcasted_iota(jnp.int32, (cells, 2 * LANES), 0)
        return total + dot_nt(left, hot.astype(BF16))

    blocks = devices * quarters
    total = lax.fori_loop(0, blocks // 2, step, jnp.zeros((120, cells), F32), unroll=4)
    total = total[0:40] + total[40:80] + total[80:120]
    region = lax.axis_index("region")
    here = centers_ref[:, pl.ds(pl.multiple_of(region * cells, cells), cells)]
    charge = total[0:6]
    n = [total[6:7], total[7:8], total[32:33]]
    none = jnp.zeros((1, cells), F32)
    fold = [
        [n[0], none, none, 0.5 * n[1], 0.5 * n[2], none],
        [none, n[1], none, 0.5 * n[0], none, 0.5 * n[2]],
        [none, none, n[2], none, 0.5 * n[0], 0.5 * n[1]],
    ]
    pad = jnp.zeros((2, cells), F32)
    moment_ref[0:8, :] = jnp.concatenate([charge, pad], axis=0)
    for a in range(3):
        about = total[8 + 8 * a : 14 + 8 * a] - (here[a : a + 1, :] - middle[a]) * charge
        about = about + jnp.concatenate(fold[a], axis=0)
        moment_ref[8 + 8 * a : 16 + 8 * a, :] = jnp.concatenate([about, pad], axis=0)


def near_body(near_ref, target_ref, first_ref, second_ref, *scratch):
    squares, factors = scratch[0:2], scratch[2:4]
    steps = near_ref.shape[0] // SOURCE_ROWS // 2
    first_ref[...] = jnp.zeros_like(first_ref)
    second_ref[...] = jnp.zeros_like(second_ref)

    def rows_of(step, start, size):
        at = [(2 * step + h) * SOURCE_ROWS + start for h in range(2)]
        return [near_ref[pl.ds(i if isinstance(i, int) else pl.multiple_of(i, 8), size), :] for i in at]

    def distances(step, slot):
        left = []
        for part in rows_of(step, 0, 8):
            p = split3(part)
            left.append(jnp.transpose(jnp.concatenate([p[0], p[0], p[0], p[1], p[1], p[2]], axis=0)))
        squares[slot][...] = dot(jnp.concatenate(left, axis=0).astype(BF16), target_ref[...])

    def powers(slot):
        g1 = lax.rsqrt(squares[slot][...])
        for k, g in ((0, g1), (2, g1 * g1 * g1)):
            high = g.astype(BF16)
            factors[slot][k] = high
            factors[slot][k + 1] = (g - high.astype(F32)).astype(BF16)

    def products(step, slot):
        high, low = split2(jnp.concatenate(rows_of(step, 8, 16), axis=1))
        left = jnp.concatenate([high[0:8], low[0:8]], axis=0).astype(BF16)
        first_ref[...] += dot(left, factors[slot][0]) + dot(left, factors[slot][1])
        left = jnp.concatenate([high, low], axis=0).astype(BF16)
        second_ref[...] += dot(left, factors[slot][2]) + dot(left, factors[slot][3])

    def pipeline(first, length):
        distances(first, 0)
        distances(first + 1, 1)
        powers(0)
        for t in range(length):
            if t + 2 < length:
                distances(first + t + 2, t % 2)
            if t + 1 < length:
                powers((t + 1) % 2)
            products(first + t, t % 2)

    if steps <= PIPELINE:
        pipeline(0, steps)
    else:

        def part(i, carry):
            pipeline(i * PIPELINE, PIPELINE)
            return carry

        lax.fori_loop(0, steps // PIPELINE, part, 0)


def stacked3(x):
    return jnp.concatenate(split3(x), axis=0).astype(BF16)


def force_body(regions, m_ref, b_ref, first_ref, second_ref, far_ref, cell_hot_ref, hot_ref, *rest):
    moment_refs, out_ref = rest[:-1], rest[-1]
    cells = moment_refs[0].shape[1]
    domains = out_ref.shape[0]
    middle = middle_of(regions)
    left = [ref[8 * j : 8 * j + 8, :] for ref in moment_refs for j in range(4)]
    left = stacked3(jnp.concatenate(left, axis=1))
    field = dot(left, far_ref[...])
    field = field[:, 0:cells] + field[:, cells:]
    field = field[0:8] + field[8:16] + field[16:24]
    field = dot(stacked3(field), cell_hot_ref[...])
    field = field[0:8] + field[8:16] + field[16:24]
    first = first_ref[...]
    second = second_ref[...]
    second = second[0:16] + second[16:32]
    x = [m_ref[a : a + 1, :] - middle[a] for a in range(3)]
    q = [second[6 + a : 7 + a] for a in range(3)]
    cross = [q[i] * x[i] if i == j else 0.5 * (q[i] * x[j] + q[j] * x[i]) for i, j in SYM]
    sigma = first[0:6] + first[8:14] + (jnp.concatenate(cross, axis=0) - second[9:15]) + field[0:6]
    at = {}
    for row, (i, j) in enumerate(SYM):
        at[i, j] = at[j, i] = sigma[row : row + 1]
    b = [b_ref[a : a + 1, :] for a in range(3)]
    force = [at[i, 0] * b[0] + at[i, 1] * b[1] + at[i, 2] * b[2] for i in range(3)]
    force = jnp.concatenate(force + [jnp.zeros((5, b[0].shape[1]), F32)], axis=0)
    spread = dot(stacked3(force), hot_ref[...])
    spread = spread[0:3] + spread[8:11] + spread[16:19]
    slots = domains * LANES
    own = (spread.shape[1] - slots) // domains
    for d in range(domains):
        pieces = [spread[:, d * LANES : (d + 1) * LANES]]
        for h in range(own // LANES):
            pieces.append(spread[:, slots + d * own + h * LANES : slots + d * own + (h + 1) * LANES])
        used = 3 * len(pieces)
        pieces.append(jnp.zeros((out_ref.shape[1] - used, LANES), F32))
        out_ref[d] = jnp.concatenate(pieces, axis=0)


def collect_body(got_ref, slot_ref, node_ref):
    domains = got_ref.shape[0]
    capacity = slot_ref.shape[1] // domains
    total = jnp.sum(got_ref[...], axis=0)
    for d in range(domains):
        slot_ref[:, d * capacity : (d + 1) * capacity] = got_ref[d, 0:3, 0:capacity]
    for h in range(node_ref.shape[1] // LANES):
        node_ref[:, h * LANES : (h + 1) * LANES] = total[3 + 3 * h : 6 + 3 * h]


def body(midpoints, line_vectors, burgers, destination, node_ids, cell_ids, cell_centers):
    count = midpoints.shape[1]
    domains = lax.axis_size("domain")
    regions = lax.axis_size("region")
    cells = cell_centers.shape[1] // regions
    nodes = count // 2 * domains
    own = nodes // domains
    cell_row = cell_ids.reshape(1, count)
    dest_row = destination.reshape(1, count)
    shape = jax.ShapeDtypeStruct
    quarters = count // LANES
    inputs = (midpoints, line_vectors, burgers, cell_row)
    payload = call(
        pack_body, shape((domains, SENT * quarters, LANES), F32), inputs, 1 << 12, "pack", fetched=inputs
    )
    got = lax.all_to_all(payload, "domain", split_axis=0, concat_axis=0, tiled=True)
    far_rows = (regions - 1) * 4 * cells
    inputs = (midpoints, dest_row, node_ids, cell_row, cell_centers)
    target, hot, cell_hot, far = call(
        functools.partial(local_body, regions, domains),
        (
            pltpu.VMEM((DIST_ROWS, count), BF16),
            pltpu.VMEM((count, domains * LANES + nodes), BF16),
            pltpu.VMEM((cells, count), BF16),
            pltpu.VMEM((far_rows, 2 * cells), BF16),
        ),
        inputs,
        1 << 30,
        "local",
        fetched=inputs,
    )
    blocks = domains * quarters
    near, moments = call(
        functools.partial(source_body, regions),
        (pltpu.VMEM((blocks * SOURCE_ROWS, LANES), F32), shape((MOMENT_ROWS, cells), F32)),
        (got.reshape(domains * SENT * quarters, LANES), cell_centers),
        1 << 28,
        "sources",
    )
    others = [
        lax.ppermute(moments, "region", [(r, r ^ k) for r in range(regions)]) for k in range(1, regions)
    ]
    first, second = call(
        near_body,
        (pltpu.VMEM((FIRST_ROWS, count), F32), pltpu.VMEM((SECOND_ROWS, count), F32)),
        (near, target),
        1 << 32,
        "near",
        scratch=[pltpu.VMEM((2 * LANES, count), F32)] * 2 + [pltpu.VMEM((4, 2 * LANES, count), BF16)] * 2,
    )
    rows = -(-(3 + 3 * (own // LANES)) // 8) * 8
    outgoing = call(
        functools.partial(force_body, regions),
        shape((domains, rows, LANES), F32),
        (midpoints, burgers, first, second, far, cell_hot, hot, *others),
        1 << 28,
        "force",
    )
    arrived = lax.all_to_all(outgoing, "domain", split_axis=0, concat_axis=0, tiled=True)
    return call(
        collect_body,
        (shape((3, 2 * count), F32), shape((3, own), F32)),
        (arrived,),
        1 << 12,
        "collect",
    )


def solution(mesh):
    both = ("region", "domain")
    in_specs = (P(None, both), P(None, both), P(None, both), P(both, None), P(None, both), P(both), P())
    out_specs = (P(None, both), P(None, both))
    return jax.shard_map(body, mesh=mesh, in_specs=in_specs, out_specs=out_specs, check_vma=False)
```

```python
import functools

import jax
import jax.numpy as jnp
from jax import lax
from jax.experimental import pallas as pl
from jax.experimental.pallas import tpu as pltpu
from jax.sharding import PartitionSpec as P

CORE2 = 0.01
LANES = 128
F32 = jnp.float32
BF16 = jnp.bfloat16
SYM = ((0, 0), (1, 1), (2, 2), (0, 1), (0, 2), (1, 2))
SENT = 10
SOURCE_ROWS = 24
DIST_ROWS = 48
FIRST_ROWS, SECOND_ROWS = 16, 32
PIPELINE = 16
MOMENT_ROWS = 32
VMEM_LIMIT = 16 << 20
VMEM_SPEC = pl.BlockSpec(memory_space=pltpu.VMEM)


def rounded(x):
    return x.astype(BF16).astype(F32)


def split2(x):
    high = rounded(x)
    return high, x - high


def split3(x):
    high = rounded(x)
    rest = x - high
    middle = rounded(rest)
    return high, middle, rest - middle


def dot(left, right):
    return jnp.dot(left, right, preferred_element_type=F32)


def dot_nt(left, right):
    return lax.dot_general(left, right, (((1,), (1,)), ((), ())), preferred_element_type=F32)


def middle_of(regions):
    region = lax.axis_index("region")
    return ((region.astype(F32) + 0.5) / regions, 0.5, 0.5)


def call(body, out_shape, inputs, flops, name, scratch=(), fetched=()):
    space = pl.BlockSpec(memory_space=pltpu.HBM) if fetched else VMEM_SPEC
    if fetched:
        inputs = [pltpu.with_memory_space_constraint(x, pltpu.HBM) for x in inputs]
    scratch = list(scratch) + [pltpu.VMEM(x.shape, x.dtype) for x in fetched]
    if fetched:
        scratch.append(pltpu.SemaphoreType.DMA((len(fetched),)))
    return pl.pallas_call(
        body,
        out_shape=out_shape,
        in_specs=[space] * len(inputs),
        out_specs=jax.tree.map(lambda _: VMEM_SPEC, out_shape),
        scratch_shapes=scratch,
        cost_estimate=pl.CostEstimate(flops=flops, bytes_accessed=1 << 16, transcendentals=0),
        compiler_params=pltpu.CompilerParams(vmem_limit_bytes=VMEM_LIMIT),
        name=name,
    )(*inputs)


def fetch(sources, buffers, semaphores):
    copies = [pltpu.make_async_copy(s, t, semaphores.at[i]) for i, (s, t) in enumerate(zip(sources, buffers))]
    for copy in copies:
        copy.start()
    for copy in copies:
        copy.wait()


def pack_body(*refs):
    sources, out_ref, buffers, semaphores = refs[:4], refs[4], refs[5:9], refs[9]
    fetch(sources, buffers, semaphores)
    m_ref, l_ref, b_ref, cell_ref = buffers
    quarters = m_ref.shape[1] // LANES
    parts = [ref[...] for ref in (m_ref, l_ref, b_ref)] + [cell_ref[...].astype(F32)]
    rows = [
        part[a : a + 1, q * LANES : (q + 1) * LANES]
        for part in parts
        for a in range(part.shape[0])
        for q in range(quarters)
    ]
    block = jnp.concatenate(rows, axis=0)
    for d in range(out_ref.shape[0]):
        out_ref[d] = block


def local_body(regions, domains, *refs):
    sources, outputs, scratch, buffers, semaphores = refs[:7], refs[7:15], refs[15:19], refs[19:26], refs[26]
    fetch(sources, buffers, semaphores)
    m_ref, l_ref, b_ref, dest_ref, nodes_ref, cell_ref, centers_ref = buffers
    target_ref, hot_ref, place_ref, own_ref, cell_hot_ref, far_ref, first_ref, second_ref = outputs
    count = m_ref.shape[1]
    cells = centers_ref.shape[1] // regions
    region = lax.axis_index("region")
    middle = middle_of(regions)
    here = centers_ref[:, pl.ds(pl.multiple_of(region * cells, cells), cells)]
    for k in range(1, regions):
        other = lax.bitwise_xor(region, k)
        there = centers_ref[:, pl.ds(pl.multiple_of(other * cells, cells), cells)]
        column = jnp.transpose(jnp.concatenate([there, jnp.zeros((5, cells), F32)], axis=0))
        d = [here[a : a + 1, :] - column[:, a : a + 1] for a in range(3)]
        g1 = lax.rsqrt(d[0] * d[0] + d[1] * d[1] + d[2] * d[2] + CORE2)
        g3 = g1 * g1 * g1
        for j, factor in enumerate([g1] + [v * g3 for v in d]):
            high, low = split2(factor)
            row = ((k - 1) * 4 + j) * cells
            far_ref[row : row + cells, 0:cells] = high.astype(BF16)
            far_ref[row : row + cells, cells : 2 * cells] = low.astype(BF16)
    x = [m_ref[a : a + 1, :] - middle[a] for a in range(3)]
    parts = [split3(-2.0 * v) for v in x]
    norm = split3(x[0] * x[0] + x[1] * x[1] + x[2] * x[2] + CORE2)
    one, none, pad = jnp.ones((1, count), F32), jnp.zeros((1, count), F32), jnp.zeros((3, count), F32)
    rows = []
    for p, of_source, of_target in ((0, one, norm[0]), (1, none, norm[1]), (2, none, norm[2]), (0, one, none), (1, none, none), (0, one, none)):
        rows += [parts[0][p], parts[1][p], parts[2][p], of_source, of_target, pad]
    target_ref[...] = jnp.concatenate(rows, axis=0).astype(BF16)
    dest = dest_ref[...]
    hot = (lax.broadcasted_iota(jnp.int32, (domains, count), 0) == dest).astype(BF16)
    earlier = (
        lax.broadcasted_iota(jnp.int32, (count, count), 0)
        < lax.broadcasted_iota(jnp.int32, (count, count), 1)
    ).astype(BF16)
    before = dot(hot, earlier)
    rank = jnp.sum(before * hot.astype(F32), axis=0, keepdims=True).astype(jnp.int32)
    nodes = nodes_ref[...]
    place_ref[...] = jnp.concatenate([dest, nodes // LANES, jnp.zeros((5, count), jnp.int32)], axis=0)
    columns = jnp.concatenate([rank, nodes % LANES, jnp.zeros((5, count), jnp.int32)], axis=0)
    columns = jnp.transpose(columns.astype(F32)).astype(jnp.int32)
    lane = lax.broadcasted_iota(jnp.int32, (count, LANES), 1)
    for i in range(3):
        hot_ref[:, i * LANES : (i + 1) * LANES] = (lane == columns[:, i : i + 1]).astype(BF16)
    cell_hot_ref[...] = (lax.broadcasted_iota(jnp.int32, (cells, count), 0) == cell_ref[...]).astype(BF16)
    own_ref[...] = jnp.concatenate(x + [b_ref[...], jnp.zeros((2, count), F32)], axis=0)
    rows = source_terms(
        x,
        [l_ref[a : a + 1, :] for a in range(3)],
        [b_ref[a : a + 1, :] for a in range(3)],
        jnp.zeros((1, count), F32),
    )
    rows = jnp.concatenate(rows, axis=0)

    def rows_of(step, start, size):
        at = [(2 * step + h) * LANES for h in range(2)]
        return [rows[start : start + size, i : i + LANES] for i in at]

    first_ref[...] = jnp.zeros_like(first_ref)
    second_ref[...] = jnp.zeros_like(second_ref)
    pair_pipeline(rows_of, count // (2 * LANES), target_ref, first_ref, second_ref, scratch)


def source_terms(m, l, b, cell):
    q = [b[1] * l[2] - b[2] * l[1], b[2] * l[0] - b[0] * l[2], b[0] * l[1] - b[1] * l[0]]
    outer = [b[i] * l[i] if i == j else 0.5 * (b[i] * l[j] + b[j] * l[i]) for i, j in SYM]
    second = [q[i] * m[i] if i == j else 0.5 * (q[i] * m[j] + q[j] * m[i]) for i, j in SYM]
    norm = m[0] * m[0] + m[1] * m[1] + m[2] * m[2]
    zero, one = jnp.zeros_like(norm), jnp.ones_like(norm)
    return m + [norm, one, cell, zero, zero] + outer + q + second + [zero]


def block_of(device, quarter):
    return (device // 8 * 4 + quarter) * 8 + device % 8


def source_body(regions, got_ref, centers_ref, near_ref, moment_ref):
    quarters = 4
    sent_rows = SENT * quarters
    devices = got_ref.shape[0] // sent_rows
    cells = moment_ref.shape[1]
    middle = middle_of(regions)
    for group in range(devices // 8):
        for quarter in range(quarters):

            def value(c):
                return got_ref[pl.ds(group * 8 * sent_rows + c * quarters + quarter, 8, stride=sent_rows), :]

            first_block = block_of(group * 8, quarter)
            rows = source_terms(
                [value(a) - middle[a] for a in range(3)],
                [value(3 + a) for a in range(3)],
                [value(6 + a) for a in range(3)],
                value(9),
            )
            for f, row in enumerate(rows):
                near_ref[pl.ds(first_block * SOURCE_ROWS + f, 8, stride=SOURCE_ROWS), :] = row

    def step(i, total):
        left, rows = [], []
        for h in range(2):
            part = near_ref[pl.ds(pl.multiple_of((2 * i + h) * SOURCE_ROWS, 8), SOURCE_ROWS), :]
            plain = part[8:16]
            terms = [split3(v) for v in [plain] + [plain * part[a : a + 1] for a in range(3)] + [part[16:24]]]
            left.append(jnp.concatenate([t[p] for p in range(3) for t in terms], axis=0))
            rows.append(part[5:6])
        left = jnp.concatenate(left, axis=1).astype(BF16)
        row = jnp.concatenate(rows, axis=1).astype(jnp.int32)
        hot = row == lax.broadcasted_iota(jnp.int32, (cells, 2 * LANES), 0)
        return total + dot_nt(left, hot.astype(BF16))

    blocks = devices * quarters
    total = lax.fori_loop(0, blocks // 2, step, jnp.zeros((120, cells), F32), unroll=min(16, blocks // 2))
    total = total[0:40] + total[40:80] + total[80:120]
    region = lax.axis_index("region")
    here = centers_ref[:, pl.ds(pl.multiple_of(region * cells, cells), cells)]
    charge = total[0:6]
    n = [total[6:7], total[7:8], total[32:33]]
    none = jnp.zeros((1, cells), F32)
    fold = [
        [n[0], none, none, 0.5 * n[1], 0.5 * n[2], none],
        [none, n[1], none, 0.5 * n[0], none, 0.5 * n[2]],
        [none, none, n[2], none, 0.5 * n[0], 0.5 * n[1]],
    ]
    pad = jnp.zeros((2, cells), F32)
    moment_ref[0:8, :] = jnp.concatenate([charge, pad], axis=0)
    for a in range(3):
        about = total[8 + 8 * a : 14 + 8 * a] - (here[a : a + 1, :] - middle[a]) * charge
        about = about + jnp.concatenate(fold[a], axis=0)
        moment_ref[8 + 8 * a : 16 + 8 * a, :] = jnp.concatenate([about, pad], axis=0)


def pair_pipeline(rows_of, length, target_ref, first_ref, second_ref, scratch):
    squares, factors = scratch[0:2], scratch[2:4]

    def distances(step, slot):
        left = []
        for part in rows_of(step, 0, 8):
            p = split3(part)
            left.append(jnp.transpose(jnp.concatenate([p[0], p[0], p[0], p[1], p[1], p[2]], axis=0)))
        squares[slot][...] = dot(jnp.concatenate(left, axis=0).astype(BF16), target_ref[...])

    def powers(slot):
        g1 = lax.rsqrt(squares[slot][...])
        for k, g in ((0, g1), (2, g1 * g1 * g1)):
            high = g.astype(BF16)
            factors[slot][k] = high
            factors[slot][k + 1] = (g - high.astype(F32)).astype(BF16)

    def products(step, slot):
        high, low = split2(jnp.concatenate(rows_of(step, 8, 16), axis=1))
        left = jnp.concatenate([high[0:8], low[0:8]], axis=0).astype(BF16)
        first_ref[...] += dot(left, factors[slot][0]) + dot(left, factors[slot][1])
        left = jnp.concatenate([high, low], axis=0).astype(BF16)
        second_ref[...] += dot(left, factors[slot][2]) + dot(left, factors[slot][3])

    for t in range(min(2, length)):
        distances(t, t)
    powers(0)
    for t in range(length):
        if t + 2 < length:
            distances(t + 2, t % 2)
        if t + 1 < length:
            powers((t + 1) % 2)
        products(t, t % 2)


def other_rows(near_ref, domains, first):
    here = lax.axis_index("domain")

    def rows_of(step, start, size):
        step = first + step
        device = lax.rem(here + 1 + step // 2, domains)
        at = [block_of(device, step % 2 * 2 + h) * SOURCE_ROWS + start for h in range(2)]
        return [near_ref[pl.ds(pl.multiple_of(i, 8), size), :] for i in at]

    return rows_of


def near_body(domains, steps, near_ref, target_ref, first_in, second_in, first_ref, second_ref, *scratch):
    first_ref[...] = first_in[...]
    second_ref[...] = second_in[...]
    length = max(n for n in range(1, PIPELINE + 1) if steps % n == 0)

    def run(first):
        pair_pipeline(other_rows(near_ref, domains, first), length, target_ref, first_ref, second_ref, scratch)

    if length == steps:
        run(0)
    else:

        def part(i, carry):
            run(i * length)
            return carry

        lax.fori_loop(0, steps // length, part, 0)


def stacked3(x):
    return jnp.concatenate(split3(x), axis=0).astype(BF16)


def force_body(own, steps, last, near_ref, target_ref, first_in, second_in, own_ref, far_ref, cell_hot_ref, hot_ref, place_ref, *rest):
    moment_refs, out_ref, scratch = rest[:-7], rest[-7], rest[-6:-2]
    first_ref, second_ref = rest[-2:]
    cells = moment_refs[0].shape[1]
    domains = out_ref.shape[0]
    left = [ref[8 * j : 8 * j + 8, :] for ref in moment_refs for j in range(4)]
    left = stacked3(jnp.concatenate(left, axis=1))
    field = dot(left, far_ref[...])
    field = field[:, 0:cells] + field[:, cells:]
    field = field[0:8] + field[8:16] + field[16:24]
    field = dot(stacked3(field), cell_hot_ref[...])
    field = field[0:8] + field[8:16] + field[16:24]
    first_ref[...] = first_in[...]
    second_ref[...] = second_in[...]
    rows_of = other_rows(near_ref, domains, steps - last)
    pair_pipeline(rows_of, last, target_ref, first_ref, second_ref, scratch)
    first = first_ref[...]
    second = second_ref[...]
    second = second[0:16] + second[16:32]
    x = [own_ref[a : a + 1, :] for a in range(3)]
    q = [second[6 + a : 7 + a] for a in range(3)]
    cross = [q[i] * x[i] if i == j else 0.5 * (q[i] * x[j] + q[j] * x[i]) for i, j in SYM]
    sigma = first[0:6] + first[8:14] + (jnp.concatenate(cross, axis=0) - second[9:15]) + field[0:6]
    at = {}
    for row, (i, j) in enumerate(SYM):
        at[i, j] = at[j, i] = sigma[row : row + 1]
    b = [own_ref[3 + a : 4 + a, :] for a in range(3)]
    force = [at[i, 0] * b[0] + at[i, 1] * b[1] + at[i, 2] * b[2] for i in range(3)]
    none = jnp.zeros_like(b[0])

    def spread(force, place, groups, i):
        parts = [split2(v) for v in force]
        rows = jnp.concatenate([v[0] for v in parts] + [none] + [v[1] for v in parts] + [none], axis=0)
        left = [jnp.where(place == g, rows, 0.0) for g in range(groups)]
        left = jnp.concatenate(left, axis=0).astype(BF16)
        return dot(left, hot_ref[:, i * LANES : (i + 1) * LANES])

    def joined(spread_rows, g):
        return spread_rows[8 * g : 8 * g + 3] + spread_rows[8 * g + 4 : 8 * g + 7]

    place = place_ref[...]
    half = [0.5 * v for v in force]
    halves = own // LANES
    slots = spread(force, place[0:1], domains, 0)
    ends = spread(half, place[1:2], domains * halves, 1) + spread(half, place[2:3], domains * halves, 2)
    for d in range(domains):
        pieces = [joined(slots, d)] + [joined(ends, d * halves + h) for h in range(halves)]
        for i, piece in enumerate(pieces):
            for a in range(3):
                at = (3 * i + a) * LANES
                out_ref[d, :, at : at + LANES] = piece[a : a + 1]


def collect_body(got_ref, slot_ref, node_ref):
    domains = got_ref.shape[0]
    capacity = slot_ref.shape[1] // domains
    total = jnp.sum(got_ref[:, :, 3 * LANES :], axis=0)
    for a in range(3):
        for d in range(domains):
            at = d * capacity
            slot_ref[a : a + 1, at : at + capacity] = got_ref[d, :, a * LANES : a * LANES + capacity]
        for h in range(node_ref.shape[1] // LANES):
            at = (3 * h + a) * LANES
            node_ref[a : a + 1, h * LANES : (h + 1) * LANES] = total[:, at : at + LANES]


def body(midpoints, line_vectors, burgers, destination, node_ids, cell_ids, cell_centers):
    count = midpoints.shape[1]
    domains = lax.axis_size("domain")
    regions = lax.axis_size("region")
    cells = cell_centers.shape[1] // regions
    own = count // 2
    cell_row = cell_ids.reshape(1, count)
    dest_row = destination.reshape(1, count)
    shape = jax.ShapeDtypeStruct
    quarters = count // LANES
    inputs = (midpoints, line_vectors, burgers, cell_row)
    payload = call(
        pack_body, shape((domains, SENT * quarters, LANES), F32), inputs, 1 << 12, "pack", fetched=inputs
    )
    got = lax.all_to_all(payload, "domain", split_axis=0, concat_axis=0, tiled=True)
    far_rows = (regions - 1) * 4 * cells
    pair_scratch = [pltpu.VMEM((2 * LANES, count), F32)] * 2 + [pltpu.VMEM((4, 2 * LANES, count), BF16)] * 2
    sums = (pltpu.VMEM((FIRST_ROWS, count), F32), pltpu.VMEM((SECOND_ROWS, count), F32))
    inputs = (midpoints, line_vectors, burgers, dest_row, node_ids, cell_row, cell_centers)
    target, hot, place, own_rows, cell_hot, far, first, second = call(
        functools.partial(local_body, regions, domains),
        (
            pltpu.VMEM((DIST_ROWS, count), BF16),
            pltpu.VMEM((count, 3 * LANES), BF16),
            pltpu.VMEM((8, count), jnp.int32),
            pltpu.VMEM((8, count), F32),
            pltpu.VMEM((cells, count), BF16),
            pltpu.VMEM((far_rows, 2 * cells), BF16),
        )
        + sums,
        inputs,
        1 << 30,
        "local",
        scratch=pair_scratch,
        fetched=inputs,
    )
    blocks = domains * quarters
    near, moments = call(
        functools.partial(source_body, regions),
        (pltpu.VMEM((blocks * SOURCE_ROWS, LANES), F32), shape((MOMENT_ROWS, cells), F32)),
        (got.reshape(domains * SENT * quarters, LANES), cell_centers),
        1 << 28,
        "sources",
    )
    others = [
        lax.ppermute(moments, "region", [(r, r ^ k) for r in range(regions)]) for k in range(1, regions)
    ]
    steps, last = (domains - 1) * quarters // 2, 2
    first, second = call(
        functools.partial(near_body, domains, steps - last),
        sums,
        (near, target, first, second),
        1 << 32,
        "near",
        scratch=pair_scratch,
    )
    sent = 3 * LANES + 3 * own
    outgoing = call(
        functools.partial(force_body, own, steps, last),
        shape((domains, 1, sent), F32),
        (near, target, first, second, own_rows, far, cell_hot, hot, place, *others),
        1 << 28,
        "force",
        scratch=pair_scratch + list(sums),
    )
    arrived = lax.all_to_all(outgoing, "domain", split_axis=0, concat_axis=0, tiled=True)
    return call(
        collect_body,
        (shape((3, 2 * count), F32), shape((3, own), F32)),
        (arrived,),
        1 << 12,
        "collect",
    )


def solution(mesh):
    both = ("region", "domain")
    in_specs = (P(None, both), P(None, both), P(None, both), P(both, None), P(None, both), P(both), P())
    out_specs = (P(None, both), P(None, both))
    return jax.shard_map(body, mesh=mesh, in_specs=in_specs, out_specs=out_specs, check_vma=False)
```

```python
import functools

import jax
import jax.numpy as jnp
from jax import lax
from jax.experimental import pallas as pl
from jax.experimental.pallas import tpu as pltpu
from jax.sharding import PartitionSpec as P

CORE2 = 0.01
LANES = 128
F32 = jnp.float32
BF16 = jnp.bfloat16
SYM = ((0, 0), (1, 1), (2, 2), (0, 1), (0, 2), (1, 2))
SENT = 10
SOURCE_ROWS = 24
DIST_ROWS = 48
FIRST_ROWS, SECOND_ROWS = 16, 32
PIPELINE = 16
MOMENT_ROWS = 24
VMEM_LIMIT = 16 << 20
VMEM_SPEC = pl.BlockSpec(memory_space=pltpu.VMEM)


def rounded(x):
    return x.astype(BF16).astype(F32)


def split2(x):
    high = rounded(x)
    return high, x - high


def split3(x):
    high = rounded(x)
    rest = x - high
    middle = rounded(rest)
    return high, middle, rest - middle


def dot(left, right):
    return jnp.dot(left, right, preferred_element_type=F32)


def dot_nt(left, right):
    return lax.dot_general(left, right, (((1,), (1,)), ((), ())), preferred_element_type=F32)


def middle_of(regions):
    region = lax.axis_index("region")
    return ((region.astype(F32) + 0.5) / regions, 0.5, 0.5)


def call(body, out_shape, inputs, flops, name, scratch=(), fetched=()):
    space = pl.BlockSpec(memory_space=pltpu.HBM) if fetched else VMEM_SPEC
    if fetched:
        inputs = [pltpu.with_memory_space_constraint(x, pltpu.HBM) for x in inputs]
    scratch = list(scratch) + [pltpu.VMEM(x.shape, x.dtype) for x in fetched]
    if fetched:
        scratch.append(pltpu.SemaphoreType.DMA((len(fetched),)))
    return pl.pallas_call(
        body,
        out_shape=out_shape,
        in_specs=[space] * len(inputs),
        out_specs=jax.tree.map(lambda _: VMEM_SPEC, out_shape),
        scratch_shapes=scratch,
        cost_estimate=pl.CostEstimate(flops=flops, bytes_accessed=1 << 16, transcendentals=0),
        compiler_params=pltpu.CompilerParams(vmem_limit_bytes=VMEM_LIMIT),
        name=name,
    )(*inputs)


def fetch(sources, buffers, semaphores):
    copies = [pltpu.make_async_copy(s, t, semaphores.at[i]) for i, (s, t) in enumerate(zip(sources, buffers))]
    for copy in copies:
        copy.start()
    for copy in copies:
        copy.wait()


def pack_body(*refs):
    sources, out_ref, buffers, semaphores = refs[:4], refs[4], refs[5:9], refs[9]
    fetch(sources, buffers, semaphores)
    m_ref, l_ref, b_ref, cell_ref = buffers
    quarters = m_ref.shape[1] // LANES
    parts = [ref[...] for ref in (m_ref, l_ref, b_ref)] + [cell_ref[...].astype(F32)]
    rows = [
        part[a : a + 1, q * LANES : (q + 1) * LANES]
        for part in parts
        for a in range(part.shape[0])
        for q in range(quarters)
    ]
    block = jnp.concatenate(rows, axis=0)
    for d in range(out_ref.shape[0]):
        out_ref[d] = block


def local_body(regions, domains, *refs):
    sources, outputs, scratch, buffers, semaphores = refs[:7], refs[7:15], refs[15:19], refs[19:26], refs[26]
    fetch(sources, buffers, semaphores)
    m_ref, l_ref, b_ref, dest_ref, nodes_ref, cell_ref, centers_ref = buffers
    target_ref, hot_ref, place_ref, own_ref, cell_hot_ref, far_ref, first_ref, second_ref = outputs
    count = m_ref.shape[1]
    cells = centers_ref.shape[1] // regions
    region = lax.axis_index("region")
    middle = middle_of(regions)
    here = centers_ref[:, pl.ds(pl.multiple_of(region * cells, cells), cells)]
    for k in range(1, regions):
        other = lax.bitwise_xor(region, k)
        there = centers_ref[:, pl.ds(pl.multiple_of(other * cells, cells), cells)]
        column = jnp.transpose(jnp.concatenate([there, jnp.zeros((5, cells), F32)], axis=0))
        d = [here[a : a + 1, :] - column[:, a : a + 1] for a in range(3)]
        g1 = lax.rsqrt(d[0] * d[0] + d[1] * d[1] + d[2] * d[2] + CORE2)
        g3 = g1 * g1 * g1
        for j, factor in enumerate([g1] + [v * g3 for v in d]):
            high, low = split2(factor)
            row = ((k - 1) * 4 + j) * cells
            far_ref[row : row + cells, 0:cells] = high.astype(BF16)
            far_ref[row : row + cells, cells : 2 * cells] = low.astype(BF16)
    x = [m_ref[a : a + 1, :] - middle[a] for a in range(3)]
    parts = [split3(-2.0 * v) for v in x]
    norm = split3(x[0] * x[0] + x[1] * x[1] + x[2] * x[2] + CORE2)
    one, none, pad = jnp.ones((1, count), F32), jnp.zeros((1, count), F32), jnp.zeros((3, count), F32)
    rows = []
    for p, of_source, of_target in ((0, one, norm[0]), (1, none, norm[1]), (2, none, norm[2]), (0, one, none), (1, none, none), (0, one, none)):
        rows += [parts[0][p], parts[1][p], parts[2][p], of_source, of_target, pad]
    target_ref[...] = jnp.concatenate(rows, axis=0).astype(BF16)
    dest = dest_ref[...]
    hot = (lax.broadcasted_iota(jnp.int32, (domains, count), 0) == dest).astype(BF16)
    earlier = (
        lax.broadcasted_iota(jnp.int32, (count, count), 0)
        < lax.broadcasted_iota(jnp.int32, (count, count), 1)
    ).astype(BF16)
    before = dot(hot, earlier)
    rank = jnp.sum(before * hot.astype(F32), axis=0, keepdims=True).astype(jnp.int32)
    nodes = nodes_ref[...]
    place_ref[...] = jnp.concatenate([dest, nodes // LANES, jnp.zeros((5, count), jnp.int32)], axis=0)
    columns = jnp.concatenate([rank, nodes % LANES, jnp.zeros((5, count), jnp.int32)], axis=0)
    columns = jnp.transpose(columns.astype(F32)).astype(jnp.int32)
    lane = lax.broadcasted_iota(jnp.int32, (count, LANES), 1)
    for i in range(3):
        hot_ref[:, i * LANES : (i + 1) * LANES] = (lane == columns[:, i : i + 1]).astype(BF16)
    cell_hot_ref[...] = (lax.broadcasted_iota(jnp.int32, (cells, count), 0) == cell_ref[...]).astype(BF16)
    own_ref[...] = jnp.concatenate(x + [b_ref[...], jnp.zeros((2, count), F32)], axis=0)
    rows = source_terms(
        x,
        [l_ref[a : a + 1, :] for a in range(3)],
        [b_ref[a : a + 1, :] for a in range(3)],
        jnp.zeros((1, count), F32),
    )
    rows = jnp.concatenate(rows, axis=0)

    def rows_of(step, start, size):
        at = [(2 * step + h) * LANES for h in range(2)]
        return [rows[start : start + size, i : i + LANES] for i in at]

    first_ref[...] = jnp.zeros_like(first_ref)
    second_ref[...] = jnp.zeros_like(second_ref)
    pair_pipeline(rows_of, count // (2 * LANES), target_ref, first_ref, second_ref, scratch)


def source_terms(m, l, b, cell):
    q = [b[1] * l[2] - b[2] * l[1], b[2] * l[0] - b[0] * l[2], b[0] * l[1] - b[1] * l[0]]
    outer = [b[i] * l[i] if i == j else 0.5 * (b[i] * l[j] + b[j] * l[i]) for i, j in SYM]
    second = [q[i] * m[i] if i == j else 0.5 * (q[i] * m[j] + q[j] * m[i]) for i, j in SYM]
    norm = m[0] * m[0] + m[1] * m[1] + m[2] * m[2]
    zero, one = jnp.zeros_like(norm), jnp.ones_like(norm)
    return m + [norm, one, cell, zero, zero] + outer + q + second + [zero]


def block_of(device, quarter):
    return (device // 8 * 4 + quarter) * 8 + device % 8


def source_body(regions, got_ref, centers_ref, near_ref, moment_ref):
    quarters = 4
    sent_rows = SENT * quarters
    devices = got_ref.shape[0] // sent_rows
    cells = moment_ref.shape[1]
    middle = middle_of(regions)
    for group in range(devices // 8):
        for quarter in range(quarters):

            def value(c):
                return got_ref[pl.ds(group * 8 * sent_rows + c * quarters + quarter, 8, stride=sent_rows), :]

            first_block = block_of(group * 8, quarter)
            rows = source_terms(
                [value(a) - middle[a] for a in range(3)],
                [value(3 + a) for a in range(3)],
                [value(6 + a) for a in range(3)],
                value(9),
            )
            for f, row in enumerate(rows):
                near_ref[pl.ds(first_block * SOURCE_ROWS + f, 8, stride=SOURCE_ROWS), :] = row

    def step(i, total):
        left, rows = [], []
        for h in range(2):
            part = near_ref[pl.ds(pl.multiple_of((2 * i + h) * SOURCE_ROWS, 8), SOURCE_ROWS), :]
            plain = part[8:16]
            terms = [split3(v) for v in [plain] + [plain * part[a : a + 1] for a in range(3)] + [part[16:24]]]
            left.append(jnp.concatenate([t[p] for p in range(3) for t in terms], axis=0))
            rows.append(part[5:6])
        left = jnp.concatenate(left, axis=1).astype(BF16)
        row = jnp.concatenate(rows, axis=1).astype(jnp.int32)
        hot = row == lax.broadcasted_iota(jnp.int32, (cells, 2 * LANES), 0)
        return total + dot_nt(left, hot.astype(BF16))

    blocks = devices * quarters
    total = lax.fori_loop(0, blocks // 2, step, jnp.zeros((120, cells), F32), unroll=min(16, blocks // 2))
    total = total[0:40] + total[40:80] + total[80:120]
    region = lax.axis_index("region")
    here = centers_ref[:, pl.ds(pl.multiple_of(region * cells, cells), cells)]
    charge = total[0:6]
    n = [total[6:7], total[7:8], total[32:33]]
    none = jnp.zeros((1, cells), F32)
    fold = [
        [n[0], none, none, 0.5 * n[1], 0.5 * n[2], none],
        [none, n[1], none, 0.5 * n[0], none, 0.5 * n[2]],
        [none, none, n[2], none, 0.5 * n[0], 0.5 * n[1]],
    ]
    groups = [charge]
    for a in range(3):
        about = total[8 + 8 * a : 14 + 8 * a] - (here[a : a + 1, :] - middle[a]) * charge
        groups.append(about + jnp.concatenate(fold[a], axis=0))
    moment_ref[...] = jnp.concatenate(groups, axis=0)


def pair_pipeline(rows_of, length, target_ref, first_ref, second_ref, scratch):
    squares, factors = scratch[0:2], scratch[2:4]

    wide = 256
    halves = target_ref.shape[1] // wide

    def distances(unit, slot):
        step, at = unit // halves, unit % halves * wide
        left = []
        for part in rows_of(step, 0, 8):
            p = split3(part)
            left.append(jnp.transpose(jnp.concatenate([p[0], p[0], p[0], p[1], p[1], p[2]], axis=0)))
        left = jnp.concatenate(left, axis=0).astype(BF16)
        squares[slot][:, 0:wide] = dot(left, target_ref[:, at : at + wide])

    def powers(slot):
        g1 = lax.rsqrt(squares[slot][:, 0:wide])
        for k, g in ((0, g1), (2, g1 * g1 * g1)):
            high = g.astype(BF16)
            factors[slot][k, :, 0:wide] = high
            factors[slot][k + 1, :, 0:wide] = (g - high.astype(F32)).astype(BF16)

    def products(unit, slot):
        step, at = unit // halves, unit % halves * wide
        f = [factors[slot][k, :, 0:wide] for k in range(4)]
        high, low = split2(jnp.concatenate(rows_of(step, 8, 16), axis=1))
        left = jnp.concatenate([high[0:8], low[0:8]], axis=0).astype(BF16)
        first_ref[:, at : at + wide] += dot(left, f[0]) + dot(left, f[1])
        left = jnp.concatenate([high, low], axis=0).astype(BF16)
        second_ref[:, at : at + wide] += dot(left, f[2]) + dot(left, f[3])

    units = length * halves
    for t in range(min(2, units)):
        distances(t, t)
    powers(0)
    for t in range(units):
        if t + 2 < units:
            distances(t + 2, t % 2)
        if t + 1 < units:
            powers((t + 1) % 2)
        products(t, t % 2)


def other_rows(near_ref, domains, first):
    here = lax.axis_index("domain")

    def rows_of(step, start, size):
        step = first + step
        device = lax.rem(here + 1 + step // 2, domains)
        at = [block_of(device, step % 2 * 2 + h) * SOURCE_ROWS + start for h in range(2)]
        return [near_ref[pl.ds(pl.multiple_of(i, 8), size), :] for i in at]

    return rows_of


def near_body(domains, steps, near_ref, target_ref, first_in, second_in, first_ref, second_ref, *scratch):
    first_ref[...] = first_in[...]
    second_ref[...] = second_in[...]
    length = max(n for n in range(1, PIPELINE + 1) if steps % n == 0)

    def run(first):
        pair_pipeline(other_rows(near_ref, domains, first), length, target_ref, first_ref, second_ref, scratch)

    if length == steps:
        run(0)
    else:

        def part(i, carry):
            run(i * length)
            return carry

        lax.fori_loop(0, steps // length, part, 0)


def stacked3(x):
    return jnp.concatenate(split3(x), axis=0).astype(BF16)


def force_body(own, steps, last, near_ref, target_ref, first_in, second_in, own_ref, far_ref, cell_hot_ref, hot_ref, place_ref, *rest):
    moment_refs, out_ref, scratch = rest[:-7], rest[-7], rest[-6:-2]
    first_ref, second_ref = rest[-2:]
    cells = moment_refs[0].shape[1]
    domains = out_ref.shape[0]
    left = [ref[6 * j : 6 * j + 6, :] for ref in moment_refs for j in range(4)]
    left = jnp.concatenate(left, axis=1)
    left = stacked3(jnp.concatenate([left, jnp.zeros((2, left.shape[1]), F32)], axis=0))
    field = dot(left, far_ref[...])
    field = field[:, 0:cells] + field[:, cells:]
    field = field[0:8] + field[8:16] + field[16:24]
    field = dot(stacked3(field), cell_hot_ref[...])
    field = field[0:8] + field[8:16] + field[16:24]
    first_ref[...] = first_in[...]
    second_ref[...] = second_in[...]
    rows_of = other_rows(near_ref, domains, steps - last)
    pair_pipeline(rows_of, last, target_ref, first_ref, second_ref, scratch)
    first = first_ref[...]
    second = second_ref[...]
    second = second[0:16] + second[16:32]
    x = [own_ref[a : a + 1, :] for a in range(3)]
    q = [second[6 + a : 7 + a] for a in range(3)]
    cross = [q[i] * x[i] if i == j else 0.5 * (q[i] * x[j] + q[j] * x[i]) for i, j in SYM]
    sigma = first[0:6] + first[8:14] + (jnp.concatenate(cross, axis=0) - second[9:15]) + field[0:6]
    at = {}
    for row, (i, j) in enumerate(SYM):
        at[i, j] = at[j, i] = sigma[row : row + 1]
    b = [own_ref[3 + a : 4 + a, :] for a in range(3)]
    force = [at[i, 0] * b[0] + at[i, 1] * b[1] + at[i, 2] * b[2] for i in range(3)]
    none = jnp.zeros_like(b[0])

    def spread(force, place, groups, i):
        parts = [split2(v) for v in force]
        rows = jnp.concatenate([v[0] for v in parts] + [none] + [v[1] for v in parts] + [none], axis=0)
        left = [jnp.where(place == g, rows, 0.0) for g in range(groups)]
        left = jnp.concatenate(left, axis=0).astype(BF16)
        return dot(left, hot_ref[:, i * LANES : (i + 1) * LANES])

    def joined(spread_rows, g):
        return spread_rows[8 * g : 8 * g + 3] + spread_rows[8 * g + 4 : 8 * g + 7]

    place = place_ref[...]
    half = [0.5 * v for v in force]
    halves = own // LANES
    slots = spread(force, place[0:1], domains, 0)
    ends = spread(half, place[1:2], domains * halves, 1) + spread(half, place[2:3], domains * halves, 2)
    for d in range(domains):
        pieces = [joined(slots, d)] + [joined(ends, d * halves + h) for h in range(halves)]
        for i, piece in enumerate(pieces):
            for a in range(3):
                at = (3 * i + a) * LANES
                out_ref[d, :, at : at + LANES] = piece[a : a + 1]


def collect_body(got_ref, slot_ref, node_ref):
    domains = got_ref.shape[0]
    capacity = slot_ref.shape[1] // domains
    total = jnp.sum(got_ref[:, :, 3 * LANES :], axis=0)
    for a in range(3):
        for d in range(domains):
            at = d * capacity
            slot_ref[a : a + 1, at : at + capacity] = got_ref[d, :, a * LANES : a * LANES + capacity]
        for h in range(node_ref.shape[1] // LANES):
            at = (3 * h + a) * LANES
            node_ref[a : a + 1, h * LANES : (h + 1) * LANES] = total[:, at : at + LANES]


def body(midpoints, line_vectors, burgers, destination, node_ids, cell_ids, cell_centers):
    count = midpoints.shape[1]
    domains = lax.axis_size("domain")
    regions = lax.axis_size("region")
    cells = cell_centers.shape[1] // regions
    own = count // 2
    cell_row = cell_ids.reshape(1, count)
    dest_row = destination.reshape(1, count)
    shape = jax.ShapeDtypeStruct
    quarters = count // LANES
    inputs = (midpoints, line_vectors, burgers, cell_row)
    payload = call(
        pack_body, shape((domains, SENT * quarters, LANES), F32), inputs, 1 << 12, "pack", fetched=inputs
    )
    got = lax.all_to_all(payload, "domain", split_axis=0, concat_axis=0, tiled=True)
    far_rows = (regions - 1) * 4 * cells
    pair_scratch = [pltpu.VMEM((2 * LANES, count), F32)] * 2 + [pltpu.VMEM((4, 2 * LANES, count), BF16)] * 2
    sums = (pltpu.VMEM((FIRST_ROWS, count), F32), pltpu.VMEM((SECOND_ROWS, count), F32))
    inputs = (midpoints, line_vectors, burgers, dest_row, node_ids, cell_row, cell_centers)
    target, hot, place, own_rows, cell_hot, far, first, second = call(
        functools.partial(local_body, regions, domains),
        (
            pltpu.VMEM((DIST_ROWS, count), BF16),
            pltpu.VMEM((count, 3 * LANES), BF16),
            pltpu.VMEM((8, count), jnp.int32),
            pltpu.VMEM((8, count), F32),
            pltpu.VMEM((cells, count), BF16),
            pltpu.VMEM((far_rows, 2 * cells), BF16),
        )
        + sums,
        inputs,
        1 << 30,
        "local",
        scratch=pair_scratch,
        fetched=inputs,
    )
    blocks = domains * quarters
    near, moments = call(
        functools.partial(source_body, regions),
        (pltpu.VMEM((blocks * SOURCE_ROWS, LANES), F32), shape((MOMENT_ROWS, cells), F32)),
        (got.reshape(domains * SENT * quarters, LANES), cell_centers),
        1 << 28,
        "sources",
    )
    others = [
        lax.ppermute(moments, "region", [(r, r ^ k) for r in range(regions)]) for k in range(1, regions)
    ]
    steps, last = (domains - 1) * quarters // 2, 2
    first, second = call(
        functools.partial(near_body, domains, steps - last),
        sums,
        (near, target, first, second),
        1 << 32,
        "near",
        scratch=pair_scratch,
    )
    sent = 3 * LANES + 3 * own
    outgoing = call(
        functools.partial(force_body, own, steps, last),
        shape((domains, 1, sent), F32),
        (near, target, first, second, own_rows, far, cell_hot, hot, place, *others),
        1 << 28,
        "force",
        scratch=pair_scratch + list(sums),
    )
    arrived = lax.all_to_all(outgoing, "domain", split_axis=0, concat_axis=0, tiled=True)
    return call(
        collect_body,
        (shape((3, 2 * count), F32), shape((3, own), F32)),
        (arrived,),
        1 << 12,
        "collect",
    )


def solution(mesh):
    both = ("region", "domain")
    in_specs = (P(None, both), P(None, both), P(None, both), P(both, None), P(None, both), P(both), P())
    out_specs = (P(None, both), P(None, both))
    return jax.shard_map(body, mesh=mesh, in_specs=in_specs, out_specs=out_specs, check_vma=False)
```

```python
import functools

import jax
import jax.numpy as jnp
from jax import lax
from jax.experimental import pallas as pl
from jax.experimental.pallas import tpu as pltpu
from jax.sharding import PartitionSpec as P

CORE2 = 0.01
LANES = 128
F32 = jnp.float32
BF16 = jnp.bfloat16
SYM = ((0, 0), (1, 1), (2, 2), (0, 1), (0, 2), (1, 2))
SENT = 10
SOURCE_ROWS = 24
DIST_ROWS = 48
FIRST_ROWS, SECOND_ROWS = 16, 32
PIPELINE = 16
MOMENT_ROWS = 24
VMEM_LIMIT = 16 << 20
VMEM_SPEC = pl.BlockSpec(memory_space=pltpu.VMEM)


def rounded(x):
    return x.astype(BF16).astype(F32)


def split2(x):
    high = rounded(x)
    return high, x - high


def split3(x):
    high = rounded(x)
    rest = x - high
    middle = rounded(rest)
    return high, middle, rest - middle


def dot(left, right):
    return jnp.dot(left, right, preferred_element_type=F32)


def dot_nt(left, right):
    return lax.dot_general(left, right, (((1,), (1,)), ((), ())), preferred_element_type=F32)


def middle_of(regions):
    region = lax.axis_index("region")
    return ((region.astype(F32) + 0.5) / regions, 0.5, 0.5)


def call(body, out_shape, inputs, flops, name, scratch=(), fetched=()):
    space = pl.BlockSpec(memory_space=pltpu.HBM) if fetched else VMEM_SPEC
    if fetched:
        inputs = [pltpu.with_memory_space_constraint(x, pltpu.HBM) for x in inputs]
    scratch = list(scratch) + [pltpu.VMEM(x.shape, x.dtype) for x in fetched]
    if fetched:
        scratch.append(pltpu.SemaphoreType.DMA((len(fetched),)))
    return pl.pallas_call(
        body,
        out_shape=out_shape,
        in_specs=[space] * len(inputs),
        out_specs=jax.tree.map(lambda _: VMEM_SPEC, out_shape),
        scratch_shapes=scratch,
        cost_estimate=pl.CostEstimate(flops=flops, bytes_accessed=1 << 16, transcendentals=0),
        compiler_params=pltpu.CompilerParams(vmem_limit_bytes=VMEM_LIMIT),
        name=name,
    )(*inputs)


def fetch(sources, buffers, semaphores):
    copies = [pltpu.make_async_copy(s, t, semaphores.at[i]) for i, (s, t) in enumerate(zip(sources, buffers))]
    for copy in copies:
        copy.start()
    for copy in copies:
        copy.wait()


def pack_body(*refs):
    sources, out_ref, buffers, semaphores = refs[:4], refs[4], refs[5:9], refs[9]
    fetch(sources, buffers, semaphores)
    m_ref, l_ref, b_ref, cell_ref = buffers
    quarters = m_ref.shape[1] // LANES
    parts = [ref[...] for ref in (m_ref, l_ref, b_ref)] + [cell_ref[...].astype(F32)]
    rows = [
        part[a : a + 1, q * LANES : (q + 1) * LANES]
        for part in parts
        for a in range(part.shape[0])
        for q in range(quarters)
    ]
    block = jnp.concatenate(rows, axis=0)
    for d in range(out_ref.shape[0]):
        out_ref[d] = block


def local_body(regions, domains, *refs):
    sources, outputs, scratch, buffers, semaphores = refs[:7], refs[7:15], refs[15:19], refs[19:26], refs[26]
    fetch(sources, buffers, semaphores)
    m_ref, l_ref, b_ref, dest_ref, nodes_ref, cell_ref, centers_ref = buffers
    target_ref, hot_ref, place_ref, own_ref, cell_hot_ref, far_ref, first_ref, second_ref = outputs
    count = m_ref.shape[1]
    cells = centers_ref.shape[1] // regions
    region = lax.axis_index("region")
    middle = middle_of(regions)
    here = centers_ref[:, pl.ds(pl.multiple_of(region * cells, cells), cells)]
    for k in range(1, regions):
        other = lax.bitwise_xor(region, k)
        there = centers_ref[:, pl.ds(pl.multiple_of(other * cells, cells), cells)]
        column = jnp.transpose(jnp.concatenate([there, jnp.zeros((5, cells), F32)], axis=0))
        d = [here[a : a + 1, :] - column[:, a : a + 1] for a in range(3)]
        g1 = lax.rsqrt(d[0] * d[0] + d[1] * d[1] + d[2] * d[2] + CORE2)
        g3 = g1 * g1 * g1
        for j, factor in enumerate([g1] + [v * g3 for v in d]):
            high, low = split2(factor)
            row = ((k - 1) * 4 + j) * cells
            far_ref[row : row + cells, 0:cells] = high.astype(BF16)
            far_ref[row : row + cells, cells : 2 * cells] = low.astype(BF16)
    x = [m_ref[a : a + 1, :] - middle[a] for a in range(3)]
    parts = [split3(-2.0 * v) for v in x]
    norm = split3(x[0] * x[0] + x[1] * x[1] + x[2] * x[2] + CORE2)
    one, none, pad = jnp.ones((1, count), F32), jnp.zeros((1, count), F32), jnp.zeros((3, count), F32)
    rows = []
    for p, of_source, of_target in ((0, one, norm[0]), (1, none, norm[1]), (2, none, norm[2]), (0, one, none), (1, none, none), (0, one, none)):
        rows += [parts[0][p], parts[1][p], parts[2][p], of_source, of_target, pad]
    target_ref[...] = jnp.concatenate(rows, axis=0).astype(BF16)
    dest = dest_ref[...]
    hot = (lax.broadcasted_iota(jnp.int32, (domains, count), 0) == dest).astype(BF16)
    earlier = (
        lax.broadcasted_iota(jnp.int32, (count, count), 0)
        < lax.broadcasted_iota(jnp.int32, (count, count), 1)
    ).astype(BF16)
    before = dot(hot, earlier)
    rank = jnp.sum(before * hot.astype(F32), axis=0, keepdims=True).astype(jnp.int32)
    nodes = nodes_ref[...]
    place_ref[...] = jnp.concatenate([dest, nodes // LANES, jnp.zeros((5, count), jnp.int32)], axis=0)
    columns = jnp.concatenate([rank, nodes % LANES, jnp.zeros((5, count), jnp.int32)], axis=0)
    columns = jnp.transpose(columns.astype(F32)).astype(jnp.int32)
    lane = lax.broadcasted_iota(jnp.int32, (count, LANES), 1)
    for i in range(3):
        hot_ref[:, i * LANES : (i + 1) * LANES] = (lane == columns[:, i : i + 1]).astype(BF16)
    cell_hot_ref[...] = (lax.broadcasted_iota(jnp.int32, (cells, count), 0) == cell_ref[...]).astype(BF16)
    own_ref[...] = jnp.concatenate(x + [b_ref[...], jnp.zeros((2, count), F32)], axis=0)
    rows = source_terms(
        x,
        [l_ref[a : a + 1, :] for a in range(3)],
        [b_ref[a : a + 1, :] for a in range(3)],
        jnp.zeros((1, count), F32),
    )
    rows = jnp.concatenate(rows, axis=0)

    def rows_of(step, start, size):
        at = [(2 * step + h) * LANES for h in range(2)]
        return [rows[start : start + size, i : i + LANES] for i in at]

    first_ref[...] = jnp.zeros_like(first_ref)
    second_ref[...] = jnp.zeros_like(second_ref)
    pair_pipeline(rows_of, count // (2 * LANES), target_ref, first_ref, second_ref, scratch)


def source_terms(m, l, b, cell):
    q = [b[1] * l[2] - b[2] * l[1], b[2] * l[0] - b[0] * l[2], b[0] * l[1] - b[1] * l[0]]
    outer = [b[i] * l[i] if i == j else 0.5 * (b[i] * l[j] + b[j] * l[i]) for i, j in SYM]
    second = [q[i] * m[i] if i == j else 0.5 * (q[i] * m[j] + q[j] * m[i]) for i, j in SYM]
    norm = m[0] * m[0] + m[1] * m[1] + m[2] * m[2]
    zero, one = jnp.zeros_like(norm), jnp.ones_like(norm)
    return m + [norm, one, cell, zero, zero] + outer + q + second + [zero]


def block_of(device, quarter):
    return (device // 8 * 4 + quarter) * 8 + device % 8


def source_body(regions, got_ref, centers_ref, near_ref, moment_ref):
    quarters = 4
    sent_rows = SENT * quarters
    devices = got_ref.shape[0] // sent_rows
    cells = moment_ref.shape[1]
    middle = middle_of(regions)
    for group in range(devices // 8):
        for quarter in range(quarters):

            def value(c):
                return got_ref[pl.ds(group * 8 * sent_rows + c * quarters + quarter, 8, stride=sent_rows), :]

            first_block = block_of(group * 8, quarter)
            rows = source_terms(
                [value(a) - middle[a] for a in range(3)],
                [value(3 + a) for a in range(3)],
                [value(6 + a) for a in range(3)],
                value(9),
            )
            for f, row in enumerate(rows):
                near_ref[pl.ds(first_block * SOURCE_ROWS + f, 8, stride=SOURCE_ROWS), :] = row

    def step(i, total):
        left, rows = [], []
        for h in range(2):
            part = near_ref[pl.ds(pl.multiple_of((2 * i + h) * SOURCE_ROWS, 8), SOURCE_ROWS), :]
            plain = part[8:16]
            terms = [split3(v) for v in [plain] + [plain * part[a : a + 1] for a in range(3)] + [part[16:24]]]
            left.append(jnp.concatenate([t[p] for p in range(3) for t in terms], axis=0))
            rows.append(part[5:6])
        left = jnp.concatenate(left, axis=1).astype(BF16)
        row = jnp.concatenate(rows, axis=1).astype(jnp.int32)
        hot = row == lax.broadcasted_iota(jnp.int32, (cells, 2 * LANES), 0)
        return total + dot_nt(left, hot.astype(BF16))

    blocks = devices * quarters
    total = lax.fori_loop(0, blocks // 2, step, jnp.zeros((120, cells), F32), unroll=min(16, blocks // 2))
    total = total[0:40] + total[40:80] + total[80:120]
    region = lax.axis_index("region")
    here = centers_ref[:, pl.ds(pl.multiple_of(region * cells, cells), cells)]
    charge = total[0:6]
    n = [total[6:7], total[7:8], total[32:33]]
    none = jnp.zeros((1, cells), F32)
    fold = [
        [n[0], none, none, 0.5 * n[1], 0.5 * n[2], none],
        [none, n[1], none, 0.5 * n[0], none, 0.5 * n[2]],
        [none, none, n[2], none, 0.5 * n[0], 0.5 * n[1]],
    ]
    groups = [charge]
    for a in range(3):
        about = total[8 + 8 * a : 14 + 8 * a] - (here[a : a + 1, :] - middle[a]) * charge
        groups.append(about + jnp.concatenate(fold[a], axis=0))
    moment_ref[...] = jnp.concatenate(groups, axis=0)


def pair_pipeline(rows_of, length, target_ref, first_ref, second_ref, scratch):
    squares, factors = scratch[0:2], scratch[2:4]

    wide = 256
    halves = target_ref.shape[1] // wide

    def distances(unit, slot):
        step, at = unit // halves, unit % halves * wide
        left = []
        for part in rows_of(step, 0, 8):
            p = split3(part)
            left.append(jnp.transpose(jnp.concatenate([p[0], p[0], p[0], p[1], p[1], p[2]], axis=0)))
        left = jnp.concatenate(left, axis=0).astype(BF16)
        squares[slot][:, 0:wide] = dot(left, target_ref[:, at : at + wide])

    def powers(slot):
        g1 = lax.rsqrt(squares[slot][:, 0:wide])
        for k, g in ((0, g1), (2, g1 * g1 * g1)):
            high = g.astype(BF16)
            factors[slot][k, :, 0:wide] = high
            factors[slot][k + 1, :, 0:wide] = (g - high.astype(F32)).astype(BF16)

    def products(unit, slot):
        step, at = unit // halves, unit % halves * wide
        f = [factors[slot][k, :, 0:wide] for k in range(4)]
        high, low = split2(jnp.concatenate(rows_of(step, 8, 16), axis=1))
        left = jnp.concatenate([high[0:8], low[0:8]], axis=0).astype(BF16)
        first_ref[:, at : at + wide] += dot(left, f[0]) + dot(left, f[1])
        left = jnp.concatenate([high, low], axis=0).astype(BF16)
        second_ref[:, at : at + wide] += dot(left, f[2]) + dot(left, f[3])

    units = length * halves
    for t in range(min(2, units)):
        distances(t, t)
    powers(0)
    for t in range(units):
        if t + 2 < units:
            distances(t + 2, t % 2)
        if t + 1 < units:
            powers((t + 1) % 2)
        products(t, t % 2)


def other_rows(near_ref, domains, first):
    here = lax.axis_index("domain")

    def rows_of(step, start, size):
        step = first + step
        device = lax.rem(here + 1 + step // 2, domains)
        at = [block_of(device, step % 2 * 2 + h) * SOURCE_ROWS + start for h in range(2)]
        return [near_ref[pl.ds(pl.multiple_of(i, 8), size), :] for i in at]

    return rows_of


def near_body(domains, steps, near_ref, target_ref, first_in, second_in, first_ref, second_ref, *scratch):
    first_ref[...] = first_in[...]
    second_ref[...] = second_in[...]
    length = max(n for n in range(1, PIPELINE + 1) if steps % n == 0)

    def run(first):
        pair_pipeline(other_rows(near_ref, domains, first), length, target_ref, first_ref, second_ref, scratch)

    if length == steps:
        run(0)
    else:

        def part(i, carry):
            run(i * length)
            return carry

        lax.fori_loop(0, steps // length, part, 0)


def stacked3(x):
    return jnp.concatenate(split3(x), axis=0).astype(BF16)


def force_body(own, order, steps, last, near_ref, target_ref, first_in, second_in, own_ref, far_ref, cell_hot_ref, hot_ref, place_ref, *rest):
    moment_refs, out_ref, scratch = rest[:-7], rest[-7], rest[-6:-2]
    first_ref, second_ref = rest[-2:]
    cells = moment_refs[0].shape[1]
    domains = out_ref.shape[0]
    left = [ref[6 * j : 6 * j + 6, :] for k in sorted(order) for ref in [moment_refs[order.index(k)]] for j in range(4)]
    left = jnp.concatenate(left, axis=1)
    left = stacked3(jnp.concatenate([left, jnp.zeros((2, left.shape[1]), F32)], axis=0))
    field = dot(left, far_ref[...])
    field = field[:, 0:cells] + field[:, cells:]
    field = field[0:8] + field[8:16] + field[16:24]
    field = dot(stacked3(field), cell_hot_ref[...])
    field = field[0:8] + field[8:16] + field[16:24]
    first_ref[...] = first_in[...]
    second_ref[...] = second_in[...]
    rows_of = other_rows(near_ref, domains, steps - last)
    pair_pipeline(rows_of, last, target_ref, first_ref, second_ref, scratch)
    first = first_ref[...]
    second = second_ref[...]
    second = second[0:16] + second[16:32]
    x = [own_ref[a : a + 1, :] for a in range(3)]
    q = [second[6 + a : 7 + a] for a in range(3)]
    cross = [q[i] * x[i] if i == j else 0.5 * (q[i] * x[j] + q[j] * x[i]) for i, j in SYM]
    sigma = first[0:6] + first[8:14] + (jnp.concatenate(cross, axis=0) - second[9:15]) + field[0:6]
    at = {}
    for row, (i, j) in enumerate(SYM):
        at[i, j] = at[j, i] = sigma[row : row + 1]
    b = [own_ref[3 + a : 4 + a, :] for a in range(3)]
    force = [at[i, 0] * b[0] + at[i, 1] * b[1] + at[i, 2] * b[2] for i in range(3)]
    none = jnp.zeros_like(b[0])

    def spread(force, place, groups, i):
        parts = [split2(v) for v in force]
        rows = jnp.concatenate([v[0] for v in parts] + [none] + [v[1] for v in parts] + [none], axis=0)
        left = [jnp.where(place == g, rows, 0.0) for g in range(groups)]
        left = jnp.concatenate(left, axis=0).astype(BF16)
        return dot(left, hot_ref[:, i * LANES : (i + 1) * LANES])

    def joined(spread_rows, g):
        return spread_rows[8 * g : 8 * g + 3] + spread_rows[8 * g + 4 : 8 * g + 7]

    place = place_ref[...]
    half = [0.5 * v for v in force]
    halves = own // LANES
    slots = spread(force, place[0:1], domains, 0)
    ends = spread(half, place[1:2], domains * halves, 1) + spread(half, place[2:3], domains * halves, 2)
    for d in range(domains):
        pieces = [joined(slots, d)] + [joined(ends, d * halves + h) for h in range(halves)]
        for i, piece in enumerate(pieces):
            for a in range(3):
                at = (3 * i + a) * LANES
                out_ref[d, :, at : at + LANES] = piece[a : a + 1]


def collect_body(got_ref, slot_ref, node_ref):
    domains = got_ref.shape[0]
    capacity = slot_ref.shape[1] // domains
    total = jnp.sum(got_ref[:, :, 3 * LANES :], axis=0)
    for a in range(3):
        for d in range(domains):
            at = d * capacity
            slot_ref[a : a + 1, at : at + capacity] = got_ref[d, :, a * LANES : a * LANES + capacity]
        for h in range(node_ref.shape[1] // LANES):
            at = (3 * h + a) * LANES
            node_ref[a : a + 1, h * LANES : (h + 1) * LANES] = total[:, at : at + LANES]


def body(midpoints, line_vectors, burgers, destination, node_ids, cell_ids, cell_centers):
    count = midpoints.shape[1]
    domains = lax.axis_size("domain")
    regions = lax.axis_size("region")
    cells = cell_centers.shape[1] // regions
    own = count // 2
    cell_row = cell_ids.reshape(1, count)
    dest_row = destination.reshape(1, count)
    shape = jax.ShapeDtypeStruct
    quarters = count // LANES
    inputs = (midpoints, line_vectors, burgers, cell_row)
    payload = call(
        pack_body, shape((domains, SENT * quarters, LANES), F32), inputs, 1 << 12, "pack", fetched=inputs
    )
    got = lax.all_to_all(payload, "domain", split_axis=0, concat_axis=0, tiled=True)
    far_rows = (regions - 1) * 4 * cells
    pair_scratch = [pltpu.VMEM((2 * LANES, count), F32)] * 2 + [pltpu.VMEM((4, 2 * LANES, count), BF16)] * 2
    sums = (pltpu.VMEM((FIRST_ROWS, count), F32), pltpu.VMEM((SECOND_ROWS, count), F32))
    inputs = (midpoints, line_vectors, burgers, dest_row, node_ids, cell_row, cell_centers)
    target, hot, place, own_rows, cell_hot, far, first, second = call(
        functools.partial(local_body, regions, domains),
        (
            pltpu.VMEM((DIST_ROWS, count), BF16),
            pltpu.VMEM((count, 3 * LANES), BF16),
            pltpu.VMEM((8, count), jnp.int32),
            pltpu.VMEM((8, count), F32),
            pltpu.VMEM((cells, count), BF16),
            pltpu.VMEM((far_rows, 2 * cells), BF16),
        )
        + sums,
        inputs,
        1 << 30,
        "local",
        scratch=pair_scratch,
        fetched=inputs,
    )
    blocks = domains * quarters
    near, moments = call(
        functools.partial(source_body, regions),
        (pltpu.VMEM((blocks * SOURCE_ROWS, LANES), F32), shape((MOMENT_ROWS, cells), F32)),
        (got.reshape(domains * SENT * quarters, LANES), cell_centers),
        1 << 28,
        "sources",
    )
    order = sorted(range(1, regions), key=lambda k: -k)
    others = [lax.ppermute(moments, "region", [(r, r ^ k) for r in range(regions)]) for k in order]
    steps, last = (domains - 1) * quarters // 2, 2
    first, second = call(
        functools.partial(near_body, domains, steps - last),
        sums,
        (near, target, first, second),
        1 << 32,
        "near",
        scratch=pair_scratch,
    )
    sent = 3 * LANES + 3 * own
    outgoing = call(
        functools.partial(force_body, own, order, steps, last),
        shape((domains, 1, sent), F32),
        (near, target, first, second, own_rows, far, cell_hot, hot, place, *others),
        1 << 28,
        "force",
        scratch=pair_scratch + list(sums),
    )
    arrived = lax.all_to_all(outgoing, "domain", split_axis=0, concat_axis=0, tiled=True)
    return call(
        collect_body,
        (shape((3, 2 * count), F32), shape((3, own), F32)),
        (arrived,),
        1 << 12,
        "collect",
    )


def solution(mesh):
    both = ("region", "domain")
    in_specs = (P(None, both), P(None, both), P(None, both), P(both, None), P(None, both), P(both), P())
    out_specs = (P(None, both), P(None, both))
    return jax.shard_map(body, mesh=mesh, in_specs=in_specs, out_specs=out_specs, check_vma=False)
```

```python
import functools

import jax
import jax.numpy as jnp
from jax import lax
from jax.experimental import pallas as pl
from jax.experimental.pallas import tpu as pltpu
from jax.sharding import PartitionSpec as P

CORE2 = 0.01
LANES = 128
F32 = jnp.float32
BF16 = jnp.bfloat16
SYM = ((0, 0), (1, 1), (2, 2), (0, 1), (0, 2), (1, 2))
SENT = 10
SOURCE_ROWS = 24
DIST_ROWS = 48
FIRST_ROWS, SECOND_ROWS = 16, 32
PIPELINE = 16
MOMENT_ROWS = 24
VMEM_LIMIT = 16 << 20
VMEM_SPEC = pl.BlockSpec(memory_space=pltpu.VMEM)


def rounded(x):
    return x.astype(BF16).astype(F32)


def split2(x):
    high = rounded(x)
    return high, x - high


def split3(x):
    high = rounded(x)
    rest = x - high
    middle = rounded(rest)
    return high, middle, rest - middle


def dot(left, right):
    return jnp.dot(left, right, preferred_element_type=F32)


def dot_nt(left, right):
    return lax.dot_general(left, right, (((1,), (1,)), ((), ())), preferred_element_type=F32)


def middle_of(regions):
    region = lax.axis_index("region")
    return ((region.astype(F32) + 0.5) / regions, 0.5, 0.5)


def call(body, out_shape, inputs, flops, name, scratch=(), fetched=()):
    space = pl.BlockSpec(memory_space=pltpu.HBM) if fetched else VMEM_SPEC
    if fetched:
        inputs = [pltpu.with_memory_space_constraint(x, pltpu.HBM) for x in inputs]
    scratch = list(scratch) + [pltpu.VMEM(x.shape, x.dtype) for x in fetched]
    if fetched:
        scratch.append(pltpu.SemaphoreType.DMA((len(fetched),)))
    return pl.pallas_call(
        body,
        out_shape=out_shape,
        in_specs=[space] * len(inputs),
        out_specs=jax.tree.map(lambda _: VMEM_SPEC, out_shape),
        scratch_shapes=scratch,
        cost_estimate=pl.CostEstimate(flops=flops, bytes_accessed=1 << 16, transcendentals=0),
        compiler_params=pltpu.CompilerParams(vmem_limit_bytes=VMEM_LIMIT),
        name=name,
    )(*inputs)


def fetch(sources, buffers, semaphores):
    copies = [pltpu.make_async_copy(s, t, semaphores.at[i]) for i, (s, t) in enumerate(zip(sources, buffers))]
    for copy in copies:
        copy.start()
    for copy in copies:
        copy.wait()


def pack_body(*refs):
    sources, out_ref, buffers, semaphores = refs[:4], refs[4], refs[5:9], refs[9]
    fetch(sources, buffers, semaphores)
    m_ref, l_ref, b_ref, cell_ref = buffers
    quarters = m_ref.shape[1] // LANES
    parts = [ref[...] for ref in (m_ref, l_ref, b_ref)] + [cell_ref[...].astype(F32)]
    rows = [
        part[a : a + 1, q * LANES : (q + 1) * LANES]
        for part in parts
        for a in range(part.shape[0])
        for q in range(quarters)
    ]
    block = jnp.concatenate(rows, axis=0)
    for d in range(out_ref.shape[0]):
        out_ref[d] = block


def local_body(regions, domains, *refs):
    sources, outputs, scratch, buffers, semaphores = refs[:7], refs[7:15], refs[15:19], refs[19:26], refs[26]
    fetch(sources, buffers, semaphores)
    m_ref, l_ref, b_ref, dest_ref, nodes_ref, cell_ref, centers_ref = buffers
    target_ref, hot_ref, place_ref, own_ref, cell_hot_ref, far_ref, first_ref, second_ref = outputs
    count = m_ref.shape[1]
    cells = centers_ref.shape[1] // regions
    region = lax.axis_index("region")
    middle = middle_of(regions)
    here = centers_ref[:, pl.ds(pl.multiple_of(region * cells, cells), cells)]
    for k in range(1, regions):
        other = lax.bitwise_xor(region, k)
        there = centers_ref[:, pl.ds(pl.multiple_of(other * cells, cells), cells)]
        column = jnp.transpose(jnp.concatenate([there, jnp.zeros((5, cells), F32)], axis=0))
        d = [here[a : a + 1, :] - column[:, a : a + 1] for a in range(3)]
        g1 = lax.rsqrt(d[0] * d[0] + d[1] * d[1] + d[2] * d[2] + CORE2)
        g3 = g1 * g1 * g1
        for j, factor in enumerate([g1] + [v * g3 for v in d]):
            high, low = split2(factor)
            row = ((k - 1) * 4 + j) * cells
            far_ref[row : row + cells, 0:cells] = high.astype(BF16)
            far_ref[row : row + cells, cells : 2 * cells] = low.astype(BF16)
    x = [m_ref[a : a + 1, :] - middle[a] for a in range(3)]
    parts = [split3(-2.0 * v) for v in x]
    norm = split3(x[0] * x[0] + x[1] * x[1] + x[2] * x[2] + CORE2)
    one, none, pad = jnp.ones((1, count), F32), jnp.zeros((1, count), F32), jnp.zeros((3, count), F32)
    rows = []
    for p, of_source, of_target in ((0, one, norm[0]), (1, none, norm[1]), (2, none, norm[2]), (0, one, none), (1, none, none), (0, one, none)):
        rows += [parts[0][p], parts[1][p], parts[2][p], of_source, of_target, pad]
    target_ref[...] = jnp.concatenate(rows, axis=0).astype(BF16)
    dest = dest_ref[...]
    hot = (lax.broadcasted_iota(jnp.int32, (domains, count), 0) == dest).astype(BF16)
    earlier = (
        lax.broadcasted_iota(jnp.int32, (count, count), 0)
        < lax.broadcasted_iota(jnp.int32, (count, count), 1)
    ).astype(BF16)
    before = dot(hot, earlier)
    rank = jnp.sum(before * hot.astype(F32), axis=0, keepdims=True).astype(jnp.int32)
    nodes = nodes_ref[...]
    place_ref[...] = jnp.concatenate([dest, nodes // LANES, jnp.zeros((5, count), jnp.int32)], axis=0)
    columns = jnp.concatenate([rank, nodes % LANES, jnp.zeros((5, count), jnp.int32)], axis=0)
    columns = jnp.transpose(columns.astype(F32)).astype(jnp.int32)
    lane = lax.broadcasted_iota(jnp.int32, (count, LANES), 1)
    for i in range(3):
        hot_ref[:, i * LANES : (i + 1) * LANES] = (lane == columns[:, i : i + 1]).astype(BF16)
    cell_hot_ref[...] = (lax.broadcasted_iota(jnp.int32, (cells, count), 0) == cell_ref[...]).astype(BF16)
    own_ref[...] = jnp.concatenate(x + [b_ref[...], jnp.zeros((2, count), F32)], axis=0)
    rows = source_terms(
        x,
        [l_ref[a : a + 1, :] for a in range(3)],
        [b_ref[a : a + 1, :] for a in range(3)],
        jnp.zeros((1, count), F32),
    )
    rows = jnp.concatenate(rows, axis=0)

    def rows_of(step, start, size):
        at = [(2 * step + h) * LANES for h in range(2)]
        return [rows[start : start + size, i : i + LANES] for i in at]

    first_ref[...] = jnp.zeros_like(first_ref)
    second_ref[...] = jnp.zeros_like(second_ref)
    pair_pipeline(rows_of, count // (2 * LANES), target_ref, first_ref, second_ref, scratch)


def source_terms(m, l, b, cell):
    q = [b[1] * l[2] - b[2] * l[1], b[2] * l[0] - b[0] * l[2], b[0] * l[1] - b[1] * l[0]]
    outer = [b[i] * l[i] if i == j else 0.5 * (b[i] * l[j] + b[j] * l[i]) for i, j in SYM]
    second = [q[i] * m[i] if i == j else 0.5 * (q[i] * m[j] + q[j] * m[i]) for i, j in SYM]
    norm = m[0] * m[0] + m[1] * m[1] + m[2] * m[2]
    zero, one = jnp.zeros_like(norm), jnp.ones_like(norm)
    return m + [norm, one, cell, zero, zero] + outer + q + second + [zero]


def block_of(device, quarter):
    return (device // 8 * 4 + quarter) * 8 + device % 8


def source_body(regions, got_ref, centers_ref, near_ref, moment_ref):
    quarters = 4
    sent_rows = SENT * quarters
    devices = got_ref.shape[0] // sent_rows
    cells = moment_ref.shape[1]
    middle = middle_of(regions)
    for group in range(devices // 8):
        for quarter in range(quarters):

            def value(c):
                return got_ref[pl.ds(group * 8 * sent_rows + c * quarters + quarter, 8, stride=sent_rows), :]

            first_block = block_of(group * 8, quarter)
            rows = source_terms(
                [value(a) - middle[a] for a in range(3)],
                [value(3 + a) for a in range(3)],
                [value(6 + a) for a in range(3)],
                value(9),
            )
            for f, row in enumerate(rows):
                near_ref[pl.ds(first_block * SOURCE_ROWS + f, 8, stride=SOURCE_ROWS), :] = row

    def step(i, total):
        left, rows = [], []
        for h in range(2):
            part = near_ref[pl.ds(pl.multiple_of((2 * i + h) * SOURCE_ROWS, 8), SOURCE_ROWS), :]
            plain = part[8:16]
            terms = [split3(v) for v in [plain] + [plain * part[a : a + 1] for a in range(3)] + [part[16:24]]]
            left.append(jnp.concatenate([t[p] for p in range(3) for t in terms], axis=0))
            rows.append(part[5:6])
        left = jnp.concatenate(left, axis=1).astype(BF16)
        row = jnp.concatenate(rows, axis=1).astype(jnp.int32)
        hot = row == lax.broadcasted_iota(jnp.int32, (cells, 2 * LANES), 0)
        return total + dot_nt(left, hot.astype(BF16))

    blocks = devices * quarters
    total = lax.fori_loop(0, blocks // 2, step, jnp.zeros((120, cells), F32), unroll=min(16, blocks // 2))
    total = total[0:40] + total[40:80] + total[80:120]
    region = lax.axis_index("region")
    here = centers_ref[:, pl.ds(pl.multiple_of(region * cells, cells), cells)]
    charge = total[0:6]
    n = [total[6:7], total[7:8], total[32:33]]
    none = jnp.zeros((1, cells), F32)
    fold = [
        [n[0], none, none, 0.5 * n[1], 0.5 * n[2], none],
        [none, n[1], none, 0.5 * n[0], none, 0.5 * n[2]],
        [none, none, n[2], none, 0.5 * n[0], 0.5 * n[1]],
    ]
    groups = [charge]
    for a in range(3):
        about = total[8 + 8 * a : 14 + 8 * a] - (here[a : a + 1, :] - middle[a]) * charge
        groups.append(about + jnp.concatenate(fold[a], axis=0))
    moment_ref[...] = jnp.concatenate(groups, axis=0)


def pair_pipeline(rows_of, length, target_ref, first_ref, second_ref, scratch):
    squares, factors = scratch[0:2], scratch[2:4]

    wide = 256
    halves = target_ref.shape[1] // wide

    def distances(unit, slot):
        step, at = unit // halves, unit % halves * wide
        left = []
        for part in rows_of(step, 0, 8):
            p = split3(part)
            left.append(jnp.transpose(jnp.concatenate([p[0], p[0], p[0], p[1], p[1], p[2]], axis=0)))
        left = jnp.concatenate(left, axis=0).astype(BF16)
        squares[slot][:, 0:wide] = dot(left, target_ref[:, at : at + wide])

    def powers(slot):
        g1 = lax.rsqrt(squares[slot][:, 0:wide])
        for k, g in ((0, g1), (2, g1 * g1 * g1)):
            high = g.astype(BF16)
            factors[slot][k, :, 0:wide] = high
            factors[slot][k + 1, :, 0:wide] = (g - high.astype(F32)).astype(BF16)

    def products(unit, slot):
        step, at = unit // halves, unit % halves * wide
        f = [factors[slot][k, :, 0:wide] for k in range(4)]
        high, low = split2(jnp.concatenate(rows_of(step, 8, 16), axis=1))
        left = jnp.concatenate([high[0:8], low[0:8]], axis=0).astype(BF16)
        first_ref[:, at : at + wide] += dot(left, f[0]) + dot(left, f[1])
        left = jnp.concatenate([high, low], axis=0).astype(BF16)
        second_ref[:, at : at + wide] += dot(left, f[2]) + dot(left, f[3])

    units = length * halves
    for t in range(min(2, units)):
        distances(t, t)
    powers(0)
    for t in range(units):
        if t + 2 < units:
            distances(t + 2, t % 2)
        if t + 1 < units:
            powers((t + 1) % 2)
        products(t, t % 2)


def other_rows(near_ref, domains, first):
    here = lax.axis_index("domain")

    def rows_of(step, start, size):
        step = first + step
        device = lax.rem(here + 1 + step // 2, domains)
        at = [block_of(device, step % 2 * 2 + h) * SOURCE_ROWS + start for h in range(2)]
        return [near_ref[pl.ds(pl.multiple_of(i, 8), size), :] for i in at]

    return rows_of


def near_body(domains, steps, near_ref, target_ref, first_in, second_in, first_ref, second_ref, *scratch):
    first_ref[...] = first_in[...]
    second_ref[...] = second_in[...]
    length = max(n for n in range(1, PIPELINE + 1) if steps % n == 0)

    def run(first):
        pair_pipeline(other_rows(near_ref, domains, first), length, target_ref, first_ref, second_ref, scratch)

    if length == steps:
        run(0)
    else:

        def part(i, carry):
            run(i * length)
            return carry

        lax.fori_loop(0, steps // length, part, 0)


def stacked3(x):
    return jnp.concatenate(split3(x), axis=0).astype(BF16)


def force_body(own, order, steps, last, near_ref, target_ref, first_in, second_in, own_ref, far_ref, cell_hot_ref, hot_ref, place_ref, *rest):
    moment_refs, out_ref, scratch = rest[:-7], rest[-7], rest[-6:-2]
    first_ref, second_ref = rest[-2:]
    cells = moment_refs[0].shape[1]
    domains = out_ref.shape[0]
    left = [ref[6 * j : 6 * j + 6, :] for k in sorted(order) for ref in [moment_refs[order.index(k)]] for j in range(4)]
    left = jnp.concatenate(left, axis=1)
    left = stacked3(jnp.concatenate([left, jnp.zeros((2, left.shape[1]), F32)], axis=0))
    field = dot(left, far_ref[...])
    field = field[:, 0:cells] + field[:, cells:]
    field = field[0:8] + field[8:16] + field[16:24]
    field = dot(stacked3(field), cell_hot_ref[...])
    field = field[0:8] + field[8:16] + field[16:24]
    first_ref[...] = first_in[...]
    second_ref[...] = second_in[...]
    rows_of = other_rows(near_ref, domains, steps - last)
    pair_pipeline(rows_of, last, target_ref, first_ref, second_ref, scratch)
    first = first_ref[...]
    second = second_ref[...]
    second = second[0:16] + second[16:32]
    x = [own_ref[a : a + 1, :] for a in range(3)]
    q = [second[6 + a : 7 + a] for a in range(3)]
    cross = [q[i] * x[i] if i == j else 0.5 * (q[i] * x[j] + q[j] * x[i]) for i, j in SYM]
    sigma = first[0:6] + first[8:14] + (jnp.concatenate(cross, axis=0) - second[9:15]) + field[0:6]
    at = {}
    for row, (i, j) in enumerate(SYM):
        at[i, j] = at[j, i] = sigma[row : row + 1]
    b = [own_ref[3 + a : 4 + a, :] for a in range(3)]
    force = [at[i, 0] * b[0] + at[i, 1] * b[1] + at[i, 2] * b[2] for i in range(3)]
    none = jnp.zeros_like(b[0])

    def spread(force, place, groups, i):
        parts = [split2(v) for v in force]
        rows = jnp.concatenate([v[0] for v in parts] + [none] + [v[1] for v in parts] + [none], axis=0)
        left = [jnp.where(place == g, rows, 0.0) for g in range(groups)]
        left = jnp.concatenate(left, axis=0).astype(BF16)
        return dot(left, hot_ref[:, i * LANES : (i + 1) * LANES])

    def joined(spread_rows, g):
        return spread_rows[8 * g : 8 * g + 3] + spread_rows[8 * g + 4 : 8 * g + 7]

    place = place_ref[...]
    half = [0.5 * v for v in force]
    halves = own // LANES
    slots = spread(force, place[0:1], domains, 0)
    ends = spread(half, place[1:2], domains * halves, 1) + spread(half, place[2:3], domains * halves, 2)
    for d in range(domains):
        pieces = [joined(slots, d)] + [joined(ends, d * halves + h) for h in range(halves)]
        for i, piece in enumerate(pieces):
            for a in range(3):
                at = (3 * i + a) * LANES
                out_ref[d, :, at : at + LANES] = piece[a : a + 1]


def collect_body(got_ref, slot_ref, node_ref):
    domains = got_ref.shape[0]
    capacity = slot_ref.shape[1] // domains
    total = jnp.sum(got_ref[:, :, 3 * LANES :], axis=0)
    for a in range(3):
        for d in range(domains):
            at = d * capacity
            slot_ref[a : a + 1, at : at + capacity] = got_ref[d, :, a * LANES : a * LANES + capacity]
        for h in range(node_ref.shape[1] // LANES):
            at = (3 * h + a) * LANES
            node_ref[a : a + 1, h * LANES : (h + 1) * LANES] = total[:, at : at + LANES]


def body(midpoints, line_vectors, burgers, destination, node_ids, cell_ids, cell_centers):
    count = midpoints.shape[1]
    domains = lax.axis_size("domain")
    regions = lax.axis_size("region")
    cells = cell_centers.shape[1] // regions
    own = count // 2
    cell_row = cell_ids.reshape(1, count)
    dest_row = destination.reshape(1, count)
    shape = jax.ShapeDtypeStruct
    quarters = count // LANES
    inputs = (midpoints, line_vectors, burgers, cell_row)
    payload = call(
        pack_body, shape((domains, SENT * quarters, LANES), F32), inputs, 1 << 12, "pack", fetched=inputs
    )
    got = lax.all_to_all(payload, "domain", split_axis=0, concat_axis=0, tiled=True)
    far_rows = (regions - 1) * 4 * cells
    pair_scratch = [pltpu.VMEM((2 * LANES, count), F32)] * 2 + [pltpu.VMEM((4, 2 * LANES, count), BF16)] * 2
    sums = (pltpu.VMEM((FIRST_ROWS, count), F32), pltpu.VMEM((SECOND_ROWS, count), F32))
    inputs = (midpoints, line_vectors, burgers, dest_row, node_ids, cell_row, cell_centers)
    target, hot, place, own_rows, cell_hot, far, first, second = call(
        functools.partial(local_body, regions, domains),
        (
            pltpu.VMEM((DIST_ROWS, count), BF16),
            pltpu.VMEM((count, 3 * LANES), BF16),
            pltpu.VMEM((8, count), jnp.int32),
            pltpu.VMEM((8, count), F32),
            pltpu.VMEM((cells, count), BF16),
            pltpu.VMEM((far_rows, 2 * cells), BF16),
        )
        + sums,
        inputs,
        1 << 30,
        "local",
        scratch=pair_scratch,
        fetched=inputs,
    )
    blocks = domains * quarters
    near, moments = call(
        functools.partial(source_body, regions),
        (pltpu.VMEM((blocks * SOURCE_ROWS, LANES), F32), shape((MOMENT_ROWS, cells), F32)),
        (got.reshape(domains * SENT * quarters, LANES), cell_centers),
        1 << 28,
        "sources",
    )
    order = sorted(range(1, regions), key=lambda k: -k)
    others = [lax.ppermute(moments, "region", [(r, r ^ k) for r in range(regions)]) for k in order]
    steps, last = (domains - 1) * quarters // 2, 4
    first, second = call(
        functools.partial(near_body, domains, steps - last),
        sums,
        (near, target, first, second),
        1 << 32,
        "near",
        scratch=pair_scratch,
    )
    sent = 3 * LANES + 3 * own
    outgoing = call(
        functools.partial(force_body, own, order, steps, last),
        shape((domains, 1, sent), F32),
        (near, target, first, second, own_rows, far, cell_hot, hot, place, *others),
        1 << 28,
        "force",
        scratch=pair_scratch + list(sums),
    )
    arrived = lax.all_to_all(outgoing, "domain", split_axis=0, concat_axis=0, tiled=True)
    return call(
        collect_body,
        (shape((3, 2 * count), F32), shape((3, own), F32)),
        (arrived,),
        1 << 12,
        "collect",
    )


def solution(mesh):
    both = ("region", "domain")
    in_specs = (P(None, both), P(None, both), P(None, both), P(both, None), P(None, both), P(both), P())
    out_specs = (P(None, both), P(None, both))
    return jax.shard_map(body, mesh=mesh, in_specs=in_specs, out_specs=out_specs, check_vma=False)
```
